16 devices in a mesh: rep: 2 (over y, z), dp: 8 (over x, core).
Axes of the slice: x: 4, y: 2, z: 1, core: 2. Of those that a mesh axis runs over, the one named last changes fastest.
The devices are a block of a 4x4x8 slice.
Arguments:
- g_w_gate: bfloat16 [16, 2, 768, 6144], P(('rep', 'dp')), parts along dimension 0
- g_w_up: bfloat16 [16, 2, 768, 6144], P(('rep', 'dp')), parts along dimension 0
- g_w_down: bfloat16 [16, 2, 6144, 768], P(('rep', 'dp')), parts along dimension 0
- w_gate: bfloat16 [2, 768, 6144], replicated
- w_up: bfloat16 [2, 768, 6144], replicated
- w_down: bfloat16 [2, 6144, 768], replicated
- m_w_gate: float32 [2, 768, 6144], P(None, 'dp')
- m_w_up: float32 [2, 768, 6144], P(None, 'dp')
- m_w_down: float32 [2, 6144, 768], P(None, 'dp')
- v_w_gate: float32 [2, 768, 6144], P(None, 'dp')
- v_w_up: float32 [2, 768, 6144], P(None, 'dp')
- v_w_down: float32 [2, 6144, 768], P(None, 'dp')
Outputs:
- output 1: bfloat16 [4, 768, 6144], P('rep'), parts along dimension 0
- output 2: bfloat16 [4, 768, 6144], P('rep'), parts along dimension 0
- output 3: bfloat16 [4, 6144, 768], P('rep'), parts along dimension 0
- output 4: float32 [4, 768, 6144], P('rep', 'dp'), parts along dimension 0
- output 5: float32 [4, 768, 6144], P('rep', 'dp'), parts along dimension 0
- output 6: float32 [4, 6144, 768], P('rep', 'dp'), parts along dimension 0
- output 7: float32 [4, 768, 6144], P('rep', 'dp'), parts along dimension 0
- output 8: float32 [4, 768, 6144], P('rep', 'dp'), parts along dimension 0
- output 9: float32 [4, 6144, 768], P('rep', 'dp'), parts along dimension 0
There are 2 independent parts. The reference program is written for one: setup_inputs(seed, part) draws one part's arguments, and reference() takes and returns one part's arrays. A program takes and returns all parts, laid end to end along the dimension named above; an argument that names none is the same for every part.
All inputs are finite; a program needn't handle non-finite values.
Results may differ from the reference program's by a relative error of at most 0.022.
Values are sent between devices in bfloat16 or wider.
A program may use at most 768 MiB of HBM per device.

```python
import jax
import jax.numpy as jnp
from jax import lax

DEVICES = 8
D = 768
FF = 6144
LAYERS = 2
NAMES = ("w_gate", "w_up", "w_down")
SHAPES = {"w_gate": (LAYERS, D, FF), "w_up": (LAYERS, D, FF), "w_down": (LAYERS, FF, D)}


def setup_inputs(seed: int = 0, part: int = 0) -> dict:
    kz, *keys = jax.random.split(jax.random.key(seed), 1 + 5 * len(NAMES))
    loud = 2.0 ** jax.random.uniform(kz, (), jnp.float32, -1.0, 1.0)
    drawn = {}
    for name, key, both in zip(NAMES, keys[:3], keys[3:6], strict=True):
        own = jax.random.normal(jax.random.fold_in(key, part), (DEVICES, *SHAPES[name]), jnp.float32)
        shared = jax.random.normal(jax.random.fold_in(both, part), SHAPES[name], jnp.float32)
        drawn["g_" + name] = (loud * (0.7 * shared / DEVICES + 0.7 * own * DEVICES**-0.5)).astype(jnp.bfloat16)
    for name, key in zip(NAMES, keys[6:9], strict=True):
        drawn[name] = (jax.random.normal(key, SHAPES[name], jnp.float32) * SHAPES[name][1] ** -0.5).astype(jnp.bfloat16)
    for name, key in zip(NAMES, keys[9:12], strict=True):
        drawn["m_" + name] = loud * 0.5 * jax.random.normal(key, SHAPES[name], jnp.float32)
    for name, key in zip(NAMES, keys[12:15], strict=True):
        drawn["v_" + name] = loud * loud * jax.random.uniform(key, SHAPES[name], jnp.float32, 0.5, 1.5)
    return drawn


def adamw(w, m, v, g):
    m = 0.9 * m + 0.1 * g
    v = 0.95 * v + 0.05 * g * g
    step = m * lax.rsqrt(v + 1e-8) + 0.1 * w
    return (w - 0.02 * step).astype(jnp.bfloat16), m, v


def reference(g_w_gate, g_w_up, g_w_down, w_gate, w_up, w_down, m_w_gate, m_w_up, m_w_down, v_w_gate, v_w_up, v_w_down):
    def total(terms):
        return lax.scan(lambda so_far, term: (so_far + term.astype(jnp.float32), None), jnp.zeros(terms.shape[1:], jnp.float32), terms)[0]

    gradients = [total(terms).astype(jnp.bfloat16).astype(jnp.float32) for terms in (g_w_gate, g_w_up, g_w_down)]
    new = [
        adamw(w.astype(jnp.float32), m, v, g)
        for w, m, v, g in zip((w_gate, w_up, w_down), (m_w_gate, m_w_up, m_w_down), (v_w_gate, v_w_up, v_w_down), gradients, strict=True)
    ]
    return tuple(one[which] for which in range(3) for one in new)
```

```python
import functools

import jax
import jax.numpy as jnp
from jax import lax
from jax.experimental import pallas as pl
from jax.experimental.pallas import tpu as pltpu
from jax.sharding import PartitionSpec as P

MESH = pl.DeviceIdType.MESH
CORES = 2
HALVES = 2
SUB = 4
DEPTH = 4
ROWS = 16
BF16, F32 = jnp.bfloat16, jnp.float32


def adamw(w, m, v, g):
    m = 0.9 * m + 0.1 * g
    v = 0.95 * v + 0.05 * g * g
    step = m * lax.rsqrt(v + 1e-8) + 0.1 * w
    return (w - 0.02 * step).astype(jnp.bfloat16), m, v


def kernel(dims, layers, n, *refs):
    kinds = 2
    it = iter(refs)

    def take(count):
        return [next(it) for _ in range(count)]

    g, w, m, v = take(3), take(3), take(3), take(3)
    w_out, m_out, v_out = take(3), take(3), take(3)
    pair, hop1, hop2 = take(3), take(3), take(3)
    own, other, r1, r2, s1, s2, mb, vb, wb = (take(kinds) for _ in range(9))
    (pair_r, hop1_r, hop2_r, near_r, far_r, core_r) = take(6)
    (pair_s, s1_s, s2_s, near_s, relay_s, last_s) = take(6)
    (own_l, other_l, r1_l, r2_l, mvw_l, mv_w, w_w) = take(7)

    chips = n // CORES
    me = lax.axis_index("dp")
    x, c = me // CORES, me % CORES
    rx, lx, ox = (x + 1) % chips, (x + chips - 1) % chips, (x + 2) % chips
    right, left, mate = {"dp": rx * CORES + c}, {"dp": lx * CORES + c}, {"dp": x * CORES + 1 - c}

    per = layers * SUB
    total = 3 * per

    def cut(W, j):
        rows, cols = dims[W]
        if W < 2:
            width = cols // SUB
            return slice(None), pl.ds(pl.multiple_of(j * width, 128), width)
        height = rows // SUB
        return pl.ds(pl.multiple_of(j * height, 16), height), slice(None)

    def at(t, f):
        for W in range(3):

            @pl.when((t >= W * per) & (t < (W + 1) * per))
            def _():
                q = t - W * per
                f(W, W // 2, q // SUB, cut(W, q % SUB))

    def remote(src, dst, send, recv, to):
        return pltpu.make_async_remote_copy(src_ref=src, dst_ref=dst, send_sem=send, recv_sem=recv, device_id=to, device_id_type=MESH)

    def local(src, dst, sem):
        return pltpu.make_async_copy(src, dst, sem)

    def landed(ref, sem):
        local(ref, ref, sem).wait()

    def sweep(kind, body):
        height, width = s1[kind].shape[-2:]
        step = width // 3
        across = width // step

        def one(q, _):
            a, b = q // across, q % across
            body(pl.ds(pl.multiple_of(a * ROWS, ROWS), ROWS), pl.ds(pl.multiple_of(b * step, 128), step))
            return 0

        lax.fori_loop(0, (height // ROWS) * across, one, 0)


    def exchange(t):
        def go(W, k, l, p):
            remote(g[W].at[l, :, 1 - c, :, *p], pair[W].at[l, :, :, *p], pair_s.at[W], pair_r.at[t], mate).start()

        at(t, go)

    def load_own(t):
        def go(W, k, l, p):
            local(g[W].at[l, :, c, :, *p], own[k].at[t % DEPTH], own_l.at[t % DEPTH]).start()

        at(t, go)

    def load_other(t):
        def go(W, k, l, p):
            landed(pair[W].at[l, :, :, *p], pair_r.at[t])
            local(pair[W].at[l, :, :, *p], other[k].at[t % DEPTH], other_l.at[t % DEPTH]).start()

        at(t, go)

    def both(k, slot, block, half, rows, cols):
        return own[k][slot, block, half, rows, cols].astype(F32) + other[k][slot, block, half, rows, cols].astype(F32)

    def first(t):
        def go(W, k, l, p):
            slot, out = t % DEPTH, t % 2
            landed(own[k].at[slot], own_l.at[slot])
            landed(other[k].at[slot], other_l.at[slot])

            @pl.when(t >= 2)
            def _():
                landed(s1[k].at[out], s1_s.at[out])

            def add(rows, cols):
                s1[k][out, 0, rows, cols] = both(k, slot, ox, 0, rows, cols).astype(BF16)
                s1[k][out, 1, rows, cols] = both(k, slot, ox, 1, rows, cols).astype(BF16)
                s1[k][out, 2, rows, cols] = both(k, slot, rx, 1, rows, cols).astype(BF16)
                s1[k][out, 3, rows, cols] = both(k, slot, lx, 0, rows, cols).astype(BF16)

            sweep(k, add)
            remote(s1[k].at[out, 0], hop1[W].at[l, 0, *p], s1_s.at[out], hop1_r.at[t], right).start()
            remote(s1[k].at[out, 1], hop1[W].at[l, 1, *p], s1_s.at[out], hop1_r.at[t], left).start()
            remote(s1[k].at[out, 2], hop2[W].at[l, 0, 1, *p], s1_s.at[out], hop2_r.at[t], right).start()
            remote(s1[k].at[out, 3], hop2[W].at[l, 1, 0, *p], s1_s.at[out], hop2_r.at[t], left).start()

        at(t, go)

    def second(t):
        def go(W, k, l, p):
            slot, out = t % DEPTH, t % 2

            @pl.when(t >= 2)
            def _():
                landed(mb[k].at[out], mv_w.at[out, 0])
                landed(vb[k].at[out], mv_w.at[out, 1])

            local(m[W].at[l, :, *p], mb[k].at[out], mvw_l.at[out, 0]).start()
            local(v[W].at[l, :, *p], vb[k].at[out], mvw_l.at[out, 1]).start()
            local(w[W].at[l, x, c, :, *p], wb[k].at[out], mvw_l.at[out, 2]).start()
            landed(hop1[W].at[l, :, *p], hop1_r.at[t])
            local(hop1[W].at[l, :, *p], r1[k], r1_l).start()

            @pl.when(t >= 2)
            def _():
                landed(s2[k].at[out], s2_s.at[out])

            landed(r1[k], r1_l)

            def add(rows, cols):
                s2[k][out, 0, rows, cols] = (both(k, slot, rx, 0, rows, cols) + r1[k][0, rows, cols].astype(F32)).astype(BF16)
                s2[k][out, 1, rows, cols] = (both(k, slot, lx, 1, rows, cols) + r1[k][1, rows, cols].astype(F32)).astype(BF16)

            sweep(k, add)
            remote(s2[k].at[out, 0], hop2[W].at[l, 0, 0, *p], s2_s.at[out], hop2_r.at[t], right).start()
            remote(s2[k].at[out, 1], hop2[W].at[l, 1, 1, *p], s2_s.at[out], hop2_r.at[t], left).start()

        at(t, go)

    def update(t):
        def go(W, k, l, p):
            slot, out = t % DEPTH, t % 2
            landed(hop2[W].at[l, :, :, *p], hop2_r.at[t])
            local(hop2[W].at[l, :, :, *p], r2[k], r2_l).start()
            landed(mb[k].at[out], mvw_l.at[out, 0])
            landed(vb[k].at[out], mvw_l.at[out, 1])
            landed(wb[k].at[out], mvw_l.at[out, 2])
            landed(r2[k], r2_l)

            def add(rows, cols):
                for h in range(HALVES):
                    place = (out, h, rows, cols)
                    total = both(k, slot, x, h, rows, cols) + r2[k][0, h, rows, cols].astype(F32) + r2[k][1, h, rows, cols].astype(F32)
                    grad = total.astype(BF16).astype(F32)
                    wb[k][place], mb[k][place], vb[k][place] = adamw(wb[k][place].astype(F32), mb[k][place], vb[k][place], grad)

            sweep(k, add)
            mine = w_out[W].at[l, x, c, :, *p]
            local(wb[k].at[out], mine, w_w).start()
            local(mb[k].at[out], m_out[W].at[l, :, *p], mv_w.at[out, 0]).start()
            local(vb[k].at[out], v_out[W].at[l, :, *p], mv_w.at[out, 1]).start()
            landed(wb[k].at[out], w_w)
            remote(mine, mine, near_s.at[W], near_r.at[t], right).start()
            remote(mine, mine, near_s.at[W], near_r.at[t], left).start()
            remote(mine, mine, near_s.at[W], core_r.at[W], mate).start()

        at(t, go)

    def relay(t):
        def go(W, k, l, p):
            landed(hop2[W].at[l, :, :, *p], near_r.at[t])
            of_left, of_right = w_out[W].at[l, lx, c, :, *p], w_out[W].at[l, rx, c, :, *p]
            half_left, half_right = w_out[W].at[l, lx, c, 0, *p], w_out[W].at[l, rx, c, 1, *p]
            remote(half_left, half_left, relay_s.at[W], far_r.at[t], right).start()
            remote(half_right, half_right, relay_s.at[W], far_r.at[t], left).start()
            remote(of_left, of_left, last_s.at[W], core_r.at[W], mate).start()
            remote(of_right, of_right, last_s.at[W], core_r.at[W], mate).start()

        at(t, go)

    def finish(t):
        def go(W, k, l, p):
            opposite = w_out[W].at[l, ox, c, :, *p]
            landed(opposite, far_r.at[t])
            remote(opposite, opposite, last_s.at[W], core_r.at[W], mate).start()

        at(t, go)


    barrier = pltpu.get_barrier_semaphore()
    for one in (right, left, mate):
        pl.semaphore_signal(barrier, inc=1, device_id=one, device_id_type=MESH)
    pl.semaphore_wait(barrier, 3)

    exchange(0)
    load_own(0)
    exchange(1)
    load_other(0)

    def round_(i, _):
        exchange(i + 2)
        load_own(i + 1)
        first(i)
        load_other(i + 1)
        second(i - 1)
        update(i - 2)
        relay(i - 3)
        finish(i - 4)
        return 0

    lax.fori_loop(0, total + 4, round_, 0)

    for t in (total - 2, total - 1):
        landed(s1[1].at[t % 2], s1_s.at[t % 2])
        landed(s2[1].at[t % 2], s2_s.at[t % 2])
        landed(mb[1].at[t % 2], mv_w.at[t % 2, 0])
        landed(vb[1].at[t % 2], mv_w.at[t % 2, 1])
    for W in range(3):
        half_of_all = w_out[W].at[:, :, 1 - c]
        landed(half_of_all, core_r.at[W])
        landed(pair[W], pair_s.at[W])
        landed(w_out[W].at[:, pl.ds(0, 3), 0], near_s.at[W])
        landed(w_out[W].at[:, 0, 0], relay_s.at[W])
        landed(w_out[W].at[:, pl.ds(0, 3), 0], last_s.at[W])


def solution(mesh):
    n = mesh.shape["dp"]

    def step(*arrays):
        terms, weights, m, v = (arrays[i : i + 3] for i in (0, 3, 6, 9))
        layers = weights[0].shape[0]
        chips = n // CORES
        assert n == CORES * chips and chips == 4
        dims = [(one.shape[1] // HALVES, one.shape[2]) for one in m]

        def whole(one, W):
            return one.reshape(layers, chips, CORES, HALVES, *dims[W])

        def block(one, W):
            return one.reshape(layers, HALVES, *dims[W])

        inputs = (
            [whole(one, W) for W, one in enumerate(terms)]
            + [whole(one, W) for W, one in enumerate(weights)]
            + [block(one, W) for W, one in enumerate(m)]
            + [block(one, W) for W, one in enumerate(v)]
        )

        def outs(*lead, dtype=BF16):
            return [jax.ShapeDtypeStruct((*lead, *dims[W]), dtype) for W in range(3)]

        out_shape = (
            outs(layers, chips, CORES, HALVES)
            + outs(layers, HALVES, dtype=F32)
            + outs(layers, HALVES, dtype=F32)
            + outs(layers, chips, HALVES)
            + outs(layers, 2)
            + outs(layers, 2, HALVES)
        )
        tiles = [(dims[0][0], dims[0][1] // SUB), (dims[2][0] // SUB, dims[2][1])]

        def vmem(*lead, dtype=BF16):
            return [pltpu.VMEM((*lead, *tile), dtype) for tile in tiles]

        dma = pltpu.SemaphoreType.DMA
        pieces = 3 * layers * SUB
        scratch = (
            vmem(DEPTH, chips, HALVES)
            + vmem(DEPTH, chips, HALVES)
            + vmem(2)
            + vmem(2, HALVES)
            + vmem(2, 4)
            + vmem(2, 2)
            + vmem(2, HALVES, dtype=F32)
            + vmem(2, HALVES, dtype=F32)
            + vmem(2, HALVES)
            + [dma((pieces,))] * 5
            + [dma((3,))]
            + [dma((3,)), dma((2,)), dma((2,)), dma((3,)), dma((3,)), dma((3,))]
            + [dma((DEPTH,)), dma((DEPTH,)), dma, dma, dma((2, 3)), dma((2, 2)), dma]
        )
        hbm = pl.BlockSpec(memory_space=pltpu.HBM)
        result = pl.pallas_call(
            functools.partial(kernel, dims, layers, n),
            out_shape=out_shape,
            in_specs=[hbm] * len(inputs),
            out_specs=[hbm] * len(out_shape),
            scratch_shapes=scratch,
            compiler_params=pltpu.CompilerParams(collective_id=0, has_side_effects=True, vmem_limit_bytes=60 * 2**20),
            name="step",
        )(*inputs)
        like = (*weights, *m, *v)
        return tuple(one.reshape(ref.shape) for one, ref in zip(result[:9], like, strict=True))

    all_of, cut = P(None, None, None), P(None, "dp", None)
    return jax.shard_map(
        step,
        mesh=mesh,
        in_specs=(P(("rep", "dp"), None, None, None),) * 3 + (all_of,) * 3 + (cut,) * 6,
        out_specs=(P("rep", None, None),) * 3 + (P("rep", "dp", None),) * 6,
        check_vma=False,
    )
```

```python
import functools
import math

import jax
import jax.numpy as jnp
from jax import lax
from jax.experimental import pallas as pl
from jax.experimental.pallas import tpu as pltpu
from jax.sharding import PartitionSpec as P


MESH = pl.DeviceIdType.MESH
CORES = 2
HALVES = 2
SUB = 4
DEPTH = 4
LAG = 4
ROWS = 16
VMEM = 67_043_328
BF16, F32 = jnp.bfloat16, jnp.float32


def adamw(w, m, v, g):
    m = 0.9 * m + 0.1 * g
    v = 0.95 * v + 0.05 * g * g
    step = m * lax.rsqrt(v + 1e-8) + 0.1 * w
    return (w - 0.02 * step).astype(jnp.bfloat16), m, v


def kernel(dims, layers, n, *refs):
    kinds = 2
    it = iter(refs)

    def take(count):
        return [next(it) for _ in range(count)]

    g, w, m, v = take(3), take(3), take(3), take(3)
    w_out, m_out, v_out = take(3), take(3), take(3)
    of_left, of_right = take(2 + layers), take(2 + layers)
    pair, hop1, hop2 = take(3), take(3), take(3)
    own, other, r1, r2, s1, s2, mb, vb, wb = (take(kinds) for _ in range(9))
    (pair_r, hop1_r, hop2_r, near_r, core_r) = take(5)
    (pair_s, s1_s, s2_s, near_s, last_s) = take(5)
    (own_l, other_l, r1_l, r2_l, mvw_l, mv_w, w_w) = take(7)

    chips = n // CORES
    me = lax.axis_index("dp")
    x, c = me // CORES, me % CORES
    rx, lx, ox = (x + 1) % chips, (x + chips - 1) % chips, (x + 2) % chips
    right, left, mate = {"dp": rx * CORES + c}, {"dp": lx * CORES + c}, {"dp": x * CORES + 1 - c}

    per = layers * SUB
    total = 3 * per

    def cut(W, j):
        rows, cols = dims[W]
        if W < 2:
            width = cols // SUB
            return slice(None), pl.ds(pl.multiple_of(j * width, 128), width)
        height = rows // SUB
        return pl.ds(pl.multiple_of(j * height, 16), height), slice(None)

    def at(t, f):
        for W in range(3):

            @pl.when((t >= W * per) & (t < (W + 1) * per))
            def _():
                q = t - W * per
                f(W, W // 2, q // SUB, cut(W, q % SUB))

    def near(t, f):
        def go(W, k, l, p):
            if W < 2:
                f(W, l, p, of_left[W].at[l, *p], of_right[W].at[l, *p])
                return
            for layer in range(layers):

                @pl.when(l == layer)
                def _():
                    f(W, layer, p, of_left[2 + layer].at[*p], of_right[2 + layer].at[*p])

        at(t, go)

    def remote(src, dst, send, recv, to):
        return pltpu.make_async_remote_copy(src_ref=src, dst_ref=dst, send_sem=send, recv_sem=recv, device_id=to, device_id_type=MESH)

    def local(src, dst, sem):
        return pltpu.make_async_copy(src, dst, sem)

    def landed(ref, sem):
        local(ref, ref, sem).wait()

    def sweep(kind, body):
        height, width = s1[kind].shape[-2:]
        step = width // 3
        across = width // step

        def one(q, _):
            a, b = q // across, q % across
            body(pl.ds(pl.multiple_of(a * ROWS, ROWS), ROWS), pl.ds(pl.multiple_of(b * step, 128), step))
            return 0

        lax.fori_loop(0, (height // ROWS) * across, one, 0)


    def exchange(t):
        def go(W, k, l, p):
            remote(g[W].at[l, :, 1 - c, :, *p], pair[W].at[l, :, :, *p], pair_s.at[W], pair_r.at[t], mate).start()

        at(t, go)

    def load_own(t):
        def go(W, k, l, p):
            local(g[W].at[l, :, c, :, *p], own[k].at[t % DEPTH], own_l.at[t % DEPTH]).start()

        at(t, go)

    def load_other(t):
        def go(W, k, l, p):
            landed(pair[W].at[l, :, :, *p], pair_r.at[t])
            local(pair[W].at[l, :, :, *p], other[k].at[t % DEPTH], other_l.at[t % DEPTH]).start()

        at(t, go)

    def both(k, slot, block, half, rows, cols):
        return own[k][slot, block, half, rows, cols].astype(F32) + other[k][slot, block, half, rows, cols].astype(F32)

    def first(t):
        def go(W, k, l, p):
            slot, out = t % DEPTH, t % 2
            landed(own[k].at[slot], own_l.at[slot])
            landed(other[k].at[slot], other_l.at[slot])

            @pl.when(t >= 2)
            def _():
                landed(s1[k].at[out], s1_s.at[out])

            def add(rows, cols):
                s1[k][out, 0, rows, cols] = both(k, slot, ox, 0, rows, cols).astype(BF16)
                s1[k][out, 1, rows, cols] = both(k, slot, ox, 1, rows, cols).astype(BF16)
                s1[k][out, 2, rows, cols] = both(k, slot, rx, 1, rows, cols).astype(BF16)
                s1[k][out, 3, rows, cols] = both(k, slot, lx, 0, rows, cols).astype(BF16)

            sweep(k, add)
            remote(s1[k].at[out, 0], hop1[W].at[l, 0, *p], s1_s.at[out], hop1_r.at[t], right).start()
            remote(s1[k].at[out, 1], hop1[W].at[l, 1, *p], s1_s.at[out], hop1_r.at[t], left).start()
            remote(s1[k].at[out, 2], hop2[W].at[l, 0, 1, *p], s1_s.at[out], hop2_r.at[t], right).start()
            remote(s1[k].at[out, 3], hop2[W].at[l, 1, 0, *p], s1_s.at[out], hop2_r.at[t], left).start()

        at(t, go)

    def second(t):
        def go(W, k, l, p):
            slot, out = t % DEPTH, t % 2

            @pl.when(t >= 2)
            def _():
                landed(mb[k].at[out], mv_w.at[out, 0])
                landed(vb[k].at[out], mv_w.at[out, 1])

            local(m[W].at[l, :, *p], mb[k].at[out], mvw_l.at[out, 0]).start()
            local(v[W].at[l, :, *p], vb[k].at[out], mvw_l.at[out, 1]).start()
            local(w[W].at[l, x, c, :, *p], wb[k].at[out], mvw_l.at[out, 2]).start()
            landed(hop1[W].at[l, :, *p], hop1_r.at[t])
            local(hop1[W].at[l, :, *p], r1[k], r1_l).start()

            @pl.when(t >= 2)
            def _():
                landed(s2[k].at[out], s2_s.at[out])

            landed(r1[k], r1_l)

            def add(rows, cols):
                s2[k][out, 0, rows, cols] = (both(k, slot, rx, 0, rows, cols) + r1[k][0, rows, cols].astype(F32)).astype(BF16)
                s2[k][out, 1, rows, cols] = (both(k, slot, lx, 1, rows, cols) + r1[k][1, rows, cols].astype(F32)).astype(BF16)

            sweep(k, add)
            remote(s2[k].at[out, 0], hop2[W].at[l, 0, 0, *p], s2_s.at[out], hop2_r.at[t], right).start()
            remote(s2[k].at[out, 1], hop2[W].at[l, 1, 1, *p], s2_s.at[out], hop2_r.at[t], left).start()

        at(t, go)

    def update(t):
        def go(W, k, l, p):
            slot, out = t % DEPTH, t % 2
            landed(hop2[W].at[l, :, :, *p], hop2_r.at[t])
            local(hop2[W].at[l, :, :, *p], r2[k], r2_l).start()
            landed(mb[k].at[out], mvw_l.at[out, 0])
            landed(vb[k].at[out], mvw_l.at[out, 1])
            landed(wb[k].at[out], mvw_l.at[out, 2])
            landed(r2[k], r2_l)

            def add(rows, cols):
                for h in range(HALVES):
                    place = (out, h, rows, cols)
                    total = both(k, slot, x, h, rows, cols) + r2[k][0, h, rows, cols].astype(F32) + r2[k][1, h, rows, cols].astype(F32)
                    grad = total.astype(BF16).astype(F32)
                    wb[k][place], mb[k][place], vb[k][place] = adamw(wb[k][place].astype(F32), mb[k][place], vb[k][place], grad)

            sweep(k, add)
            mine = w_out[W].at[l, x, c, :, *p]

            local(wb[k].at[out], mine, w_w).start()
            local(mb[k].at[out], m_out[W].at[l, :, *p], mv_w.at[out, 0]).start()
            local(vb[k].at[out], v_out[W].at[l, :, *p], mv_w.at[out, 1]).start()
            landed(wb[k].at[out], w_w)

        at(t, go)

    def spread(t):
        def go(W, l, p, from_left, from_right):
            mine, first, last = w_out[W].at[l, x, c, :, *p], w_out[W].at[l, x, c, 0, *p], w_out[W].at[l, x, c, 1, *p]
            remote(first, from_left, near_s.at[W], near_r.at[t], right).start()
            remote(last, from_right, near_s.at[W], near_r.at[t], left).start()
            remote(last, last, near_s.at[W], near_r.at[t], right).start()
            remote(first, first, near_s.at[W], near_r.at[t], left).start()
            remote(mine, mine, near_s.at[W], core_r.at[W], mate).start()

        near(t, go)

    def relay(t):
        def go(W, l, p, from_left, from_right):
            landed(hop2[W].at[l, :, :, *p], near_r.at[t])
            left0, left1 = w_out[W].at[l, lx, c, 0, *p], w_out[W].at[l, lx, c, 1, *p]
            right0, right1 = w_out[W].at[l, rx, c, 0, *p], w_out[W].at[l, rx, c, 1, *p]
            for src, dst in ((from_left, left0), (left1, left1), (right0, right0), (from_right, right1)):
                remote(src, dst, last_s.at[W], core_r.at[W], mate).start()

        near(t, go)


    barrier = pltpu.get_barrier_semaphore()
    for one in (right, left, mate):
        pl.semaphore_signal(barrier, inc=1, device_id=one, device_id_type=MESH)
    pl.semaphore_wait(barrier, 3)

    exchange(0)
    load_own(0)
    exchange(1)
    load_other(0)

    def round_(i, _):
        exchange(i + 2)
        load_own(i + 1)
        first(i)
        load_other(i + 1)
        second(i - 1)
        update(i - 2)
        spread(i - 2 - LAG)
        relay(i - 3 - LAG)
        return 0

    lax.fori_loop(0, total + 3 + LAG, round_, 0)

    for t in (total - 2, total - 1):
        landed(s1[1].at[t % 2], s1_s.at[t % 2])
        landed(s2[1].at[t % 2], s2_s.at[t % 2])
        landed(mb[1].at[t % 2], mv_w.at[t % 2, 0])
        landed(vb[1].at[t % 2], mv_w.at[t % 2, 1])
    for W in range(3):
        landed(w_out[W].at[:, pl.ds(0, 3), 0], core_r.at[W])
        landed(pair[W], pair_s.at[W])
        landed(w_out[W].at[:, pl.ds(0, 3), 0], near_s.at[W])
        landed(w_out[W].at[:, pl.ds(0, 2), 0], last_s.at[W])


def moves(sources, results, jobs, given=None):
    count, extra = len(sources), 0 if given is None else 1

    def body(*refs):
        ins, outs = refs[:count], refs[count + extra : count + extra + len(results)]
        bufs, (got, put) = refs[count + extra + len(results) : -2], refs[-2:]
        me = lax.axis_index("dp")
        x, c = me // CORES, me % CORES

        def load(q, i):
            src, _, _, slots, _, _, where = jobs[q]
            return pltpu.make_async_copy(ins[src].at[where(i, x, c)[0]], bufs[q].at[i % slots], got.at[q, i % slots])

        def store(q, i):
            _, dst, _, slots, _, _, where = jobs[q]
            return pltpu.make_async_copy(bufs[q].at[i % slots], outs[dst].at[where(i, x, c)[1]], put.at[q, i % slots])

        for i in range(max(job[4] for job in jobs)):
            for q, job in enumerate(jobs):
                if i < min(job[4], job[2]):
                    load(q, i).start()
        for i in range(max(job[2] for job in jobs)):
            for q, (_, _, steps, slots, ahead, _, _) in enumerate(jobs):
                if i < steps:
                    load(q, i).wait()
                    store(q, i).start()
                    if i + ahead < steps:
                        if i + ahead >= slots:
                            store(q, i + ahead - slots).wait()
                        load(q, i + ahead).start()
        for q, (_, _, steps, slots, _, _, _) in enumerate(jobs):
            for i in range(max(0, steps - slots), steps):
                store(q, i).wait()

    most = max(job[3] for job in jobs)
    hbm = pl.BlockSpec(memory_space=pltpu.HBM)
    nbytes = 2 * sum(job[2] * math.prod(job[5]) * sources[job[0]].dtype.itemsize for job in jobs)
    return pl.pallas_call(
        body,
        in_specs=[hbm] * (count + extra),
        out_specs=[hbm] * len(results),
        out_shape=results,
        scratch_shapes=[pltpu.VMEM((job[3], *job[5]), sources[job[0]].dtype) for job in jobs]
        + [pltpu.SemaphoreType.DMA((len(jobs), most))] * 2,
        input_output_aliases={count: 0} if extra else {},
        compiler_params=pltpu.CompilerParams(vmem_limit_bytes=VMEM),
        cost_estimate=pl.CostEstimate(flops=nbytes * 8, bytes_accessed=nbytes, transcendentals=0),
    )(*sources, *(() if given is None else (given,)))


def solution(mesh):
    n = mesh.shape["dp"]

    def update(*arrays):
        terms, weights, m, v = (arrays[i : i + 3] for i in (0, 3, 6, 9))
        layers = weights[0].shape[0]
        chips = n // CORES
        assert n == CORES * chips and chips == 4
        dims = [(one.shape[1] // HALVES, one.shape[2]) for one in m]

        def whole(one, W):
            return one.reshape(layers, chips, CORES, HALVES, *dims[W])

        def block(one, W):
            return one.reshape(layers, HALVES, *dims[W])

        inputs = (
            [whole(one, W) for W, one in enumerate(terms)]
            + [whole(one, W) for W, one in enumerate(weights)]
            + [block(one, W) for W, one in enumerate(m)]
            + [block(one, W) for W, one in enumerate(v)]
        )

        def outs(*lead, dtype=BF16):
            return [jax.ShapeDtypeStruct((*lead, *dims[W]), dtype) for W in range(3)]

        nears = outs(layers)[:2] + [jax.ShapeDtypeStruct(dims[2], BF16)] * layers
        out_shape = (
            outs(layers, chips, CORES, HALVES)
            + outs(layers, HALVES, dtype=F32)
            + outs(layers, HALVES, dtype=F32)
            + nears * 2
            + outs(layers, chips, HALVES)
            + outs(layers, 2)
            + outs(layers, 2, HALVES)
        )
        tiles = [(dims[0][0], dims[0][1] // SUB), (dims[2][0] // SUB, dims[2][1])]

        def vmem(*lead, dtype=BF16):
            return [pltpu.VMEM((*lead, *tile), dtype) for tile in tiles]

        dma = pltpu.SemaphoreType.DMA
        pieces = 3 * layers * SUB
        scratch = (
            vmem(DEPTH, chips, HALVES)
            + vmem(DEPTH, chips, HALVES)
            + vmem(2)
            + vmem(2, HALVES)
            + vmem(2, 4)
            + vmem(2, 2)
            + vmem(2, HALVES, dtype=F32)
            + vmem(2, HALVES, dtype=F32)
            + vmem(2, HALVES)
            + [dma((pieces,))] * 4
            + [dma((3,))]
            + [dma((3,)), dma((2,)), dma((2,)), dma((3,)), dma((3,))]
            + [dma((DEPTH,)), dma((DEPTH,)), dma, dma, dma((2, 3)), dma((2, 2)), dma]
        )
        hbm = pl.BlockSpec(memory_space=pltpu.HBM)
        result = pl.pallas_call(
            functools.partial(kernel, dims, layers, n),
            out_shape=out_shape,
            in_specs=[hbm] * len(inputs),
            out_specs=[hbm] * len(out_shape),
            scratch_shapes=scratch,
            compiler_params=pltpu.CompilerParams(collective_id=0, has_side_effects=True, vmem_limit_bytes=VMEM),
            name="step",
        )(*inputs)
        new_w, new_m, new_v = result[:3], result[3:6], result[6:9]
        of_left, of_right = result[9 : 9 + len(nears)], result[9 + len(nears) : 9 + 2 * len(nears)]

        def moved(one, along, other=False):
            to = [((d // CORES + along) % chips * CORES + (d % CORES + other) % CORES) for d in range(n)]
            return lax.ppermute(one, "dp", list(enumerate(to)))

        def like(one):
            return jax.ShapeDtypeStruct(one.shape, one.dtype)

        every = slice(None)

        def of_blocks(W, src, dst, blocks, half, slots, ahead):
            def where(i, x, c):
                along, other, which = blocks[i // layers]
                place = (i % layers, (x + along) % chips, 1 - c if other else c, which)
                return place, place

            return src, dst, layers * len(blocks), slots, ahead, dims[W] if half else (HALVES, *dims[W]), where

        def of_near(W, src, dst, along, other, half, layer=None, slots=2):
            cuts = 2
            shape = (dims[W][0], dims[W][1] // cuts) if W < 2 else (dims[W][0] // cuts, dims[W][1])

            def where(i, x, c):
                q = i % cuts
                at = (every, pl.ds(q * shape[1], shape[1])) if W < 2 else (pl.ds(q * shape[0], shape[0]), every)
                l = i // cuts if layer is None else layer
                return ((l, *at) if layer is None else at), (l, (x + along) % chips, 1 - c if other else c, half, *at)

            steps = cuts * (layers if layer is None else 1)
            return src, dst, steps, slots, slots // 2, shape, where

        def of_moment(W, src, dst, cuts, slots, ahead):
            shape = (dims[W][0], dims[W][1] // cuts) if W < 2 else (dims[W][0] // cuts, dims[W][1])

            def where(i, x, c):
                q = i % cuts
                at = (every, pl.ds(q * shape[1], shape[1])) if W < 2 else (pl.ds(q * shape[0], shape[0]), every)
                place = (i // (cuts * HALVES), i // cuts % HALVES, *at)
                return place, place

            return src, dst, layers * HALVES * cuts, slots, ahead, shape, where

        def copied(which, new_w, new_m, new_v, of_left, of_right):
            here = [one[W] for one in (new_w, new_m, new_v) for W in which]
            count, jobs, late = len(which), [], []
            for q, W in enumerate(which):
                full = ((0, False, every), (0, True, every), (-1, True, every), (1, True, every))
                jobs.append(of_blocks(W, q, q, full, False, 6, 3))
                jobs.append(of_blocks(W, q, q, ((-1, False, 1), (1, False, 0)), True, 4, 2))
                jobs += [of_moment(W, i, i, 2, 6, 3) for i in (count + q, 2 * count + q)]
                for layer in (None,) if W < 2 else range(layers):
                    at = W + (layer or 0)
                    for one, along, half in ((of_left, -1, 0), (of_right, 1, 1)):
                        jobs.append(of_near(W, len(here) + len(late), q, along, False, half, layer, 4))
                        late.append(one[at])
            return moves((*here, *late), [like(one) for one in here], jobs)

        def placed(W, one, halves):
            jobs = [of_near(W, i, 0, 2, other, half, layer, 4) for i, (_, other, half, layer) in enumerate(halves)]
            return moves([half[0] for half in halves], [like(one)], jobs, one)[0]

        def over(far):
            return [moved(one, 0, True) for one in far]

        def halves(far, mates, layer=None):
            return [(one, other, h, layer) for other, both in ((False, far), (True, mates)) for h, one in enumerate(both)]

        def after(far, which, *others):
            one, others = lax.optimization_barrier((far[which], others))
            return [one if i == which else old for i, old in enumerate(far)], *others

        far = []
        for a, b in zip(of_left, of_right, strict=True):
            far.append((moved(a, 1), moved(b, -1)))
        gate, up, gate_m, up_m, gate_v, up_v = copied((0, 1), new_w, new_m, new_v, of_left, of_right)
        far, _, *rest = after(far, 0, gate_m, new_w, new_m, new_v, of_left, of_right)
        gate_mate = over(far[0])
        down, down_m, down_v = copied((2,), *rest)
        far, gate_mate, _ = after(far, 1, gate_mate, down_m)
        up_mate = over(far[1])
        gate = placed(0, gate, halves(far[0], gate_mate))
        far, up_mate, gate = after(far, 2, up_mate, gate)
        down_mate = over(far[2])
        up = placed(1, up, halves(far[1], up_mate))
        for layer in range(1, layers):
            far, down_mate, up = after(far, 2 + layer, down_mate, up)
            next_mate = over(far[2 + layer])
            down = placed(2, down, halves(far[1 + layer], down_mate, layer - 1))
            down_mate = next_mate
        down = placed(2, down, halves(far[1 + layers], (), layers - 1))
        down = placed(2, down, [(one, True, h, layers - 1) for h, one in enumerate(down_mate)])

        found = (gate, up, down, gate_m, up_m, down_m, gate_v, up_v, down_v)
        return tuple(one.reshape(ref.shape) for one, ref in zip(found, (*weights, *m, *v), strict=True))

    all_of, cut = P(None, None, None), P(None, "dp", None)
    return jax.shard_map(
        update,
        mesh=mesh,
        in_specs=(P(("rep", "dp"), None, None, None),) * 3 + (all_of,) * 3 + (cut,) * 6,
        out_specs=(P("rep", None, None),) * 3 + (P("rep", "dp", None),) * 6,
        check_vma=False,
    )
```

```python
import functools
import math

import jax
import jax.numpy as jnp
from jax import lax
from jax.experimental import pallas as pl
from jax.experimental.pallas import tpu as pltpu
from jax.sharding import PartitionSpec as P


MESH = pl.DeviceIdType.MESH
CORES = 2
HALVES = 2
SUB = 4
DEPTH = 4
LAG = 4
ROWS = 16
VMEM = 67_043_328
BF16, F32 = jnp.bfloat16, jnp.float32


def adamw(w, m, v, g):
    m = 0.9 * m + 0.1 * g
    v = 0.95 * v + 0.05 * g * g
    step = m * lax.rsqrt(v + 1e-8) + 0.1 * w
    return (w - 0.02 * step).astype(jnp.bfloat16), m, v


def kernel(dims, layers, n, *refs):
    kinds = 2
    it = iter(refs)

    def take(count):
        return [next(it) for _ in range(count)]

    g, w, m, v = take(3), take(3), take(3), take(3)
    w_out, m_out, v_out = take(3), take(3), take(3)
    of_left, of_right = take(2 + layers), take(2 + layers)
    pair, hop1, hop2 = take(3), take(3), take(3)
    own, other, r1, r2, s1, s2, mb, vb, wb = (take(kinds) for _ in range(9))
    (pair_r, hop1_r, hop2_r, near_r, core_r, open_r) = take(6)
    (pair_s, s1_s, s2_s, near_s, last_s) = take(5)
    (own_l, other_l, r1_l, r2_l, mvw_l, mv_w, w_w) = take(7)

    chips = n // CORES
    me = lax.axis_index("dp")
    x, c = me // CORES, me % CORES
    rx, lx, ox = (x + 1) % chips, (x + chips - 1) % chips, (x + 2) % chips
    right, left, mate = {"dp": rx * CORES + c}, {"dp": lx * CORES + c}, {"dp": x * CORES + 1 - c}

    per = layers * SUB
    total = 3 * per

    def cut(W, j):
        rows, cols = dims[W]
        if W < 2:
            width = cols // SUB
            return slice(None), pl.ds(pl.multiple_of(j * width, 128), width)
        height = rows // SUB
        return pl.ds(pl.multiple_of(j * height, 16), height), slice(None)

    def at(t, f):
        for W in range(3):

            @pl.when((t >= W * per) & (t < (W + 1) * per))
            def _():
                q = t - W * per
                f(W, W // 2, q // SUB, cut(W, q % SUB))

    def near(t, f):
        def go(W, k, l, p):
            if W < 2:
                f(W, l, p, of_left[W].at[l, *p], of_right[W].at[l, *p])
                return
            for layer in range(layers):

                @pl.when(l == layer)
                def _():
                    f(W, layer, p, of_left[2 + layer].at[*p], of_right[2 + layer].at[*p])

        at(t, go)

    def remote(src, dst, send, recv, to):
        return pltpu.make_async_remote_copy(src_ref=src, dst_ref=dst, send_sem=send, recv_sem=recv, device_id=to, device_id_type=MESH)

    def local(src, dst, sem):
        return pltpu.make_async_copy(src, dst, sem)

    def landed(ref, sem):
        local(ref, ref, sem).wait()

    def sweep(kind, body):
        height, width = s1[kind].shape[-2:]
        step = width // 3
        across = width // step

        def one(q, _):
            a, b = q // across, q % across
            body(pl.ds(pl.multiple_of(a * ROWS, ROWS), ROWS), pl.ds(pl.multiple_of(b * step, 128), step))
            return 0

        lax.fori_loop(0, (height // ROWS) * across, one, 0)


    def exchange(t):
        def go(W, k, l, p):
            remote(g[W].at[l, :, 1 - c, :, *p], pair[W].at[l, :, :, *p], pair_s.at[W], pair_r.at[t], mate).start()

        at(t, go)

    def load_own(t):
        def go(W, k, l, p):
            local(g[W].at[l, :, c, :, *p], own[k].at[t % DEPTH], own_l.at[t % DEPTH]).start()

        at(t, go)

    def load_other(t):
        def go(W, k, l, p):
            landed(pair[W].at[l, :, :, *p], pair_r.at[t])
            local(pair[W].at[l, :, :, *p], other[k].at[t % DEPTH], other_l.at[t % DEPTH]).start()

        at(t, go)

    def both(k, slot, block, half, rows, cols):
        return own[k][slot, block, half, rows, cols].astype(F32) + other[k][slot, block, half, rows, cols].astype(F32)

    def opening():
        p = cut(0, 0)
        blocks = ((ox, (0, 1)), (rx, (2,)), (lx, (3,)), (x, ()))
        for i, (block, _) in enumerate(blocks):
            remote(g[0].at[0, block, 1 - c, :, *p], other[0].at[0, block], pair_s.at[0], open_r.at[i], mate).start()
        exchange(1)
        exchange(2)
        load_own(1)
        landed(own[0].at[0], own_l.at[0])
        halves = ((ox, 0), (ox, 1), (rx, 1), (lx, 0))
        ends = ((hop1, (0,), hop1_r, right), (hop1, (1,), hop1_r, left), (hop2, (0, 1), hop2_r, right), (hop2, (1, 0), hop2_r, left))
        for i, (block, which) in enumerate(blocks):
            landed(other[0].at[0, block], open_r.at[i])
            if which:

                def add(rows, cols):
                    for q in which:
                        s1[0][0, q, rows, cols] = both(0, 0, *halves[q], rows, cols).astype(BF16)

                sweep(0, add)
            for q in which:
                hop, place, sem, to = ends[q]
                remote(s1[0].at[0, q], hop[0].at[0, *place, *p], s1_s.at[0], sem.at[0], to).start()

    def first(t):
        def go(W, k, l, p):
            slot, out = t % DEPTH, t % 2
            landed(own[k].at[slot], own_l.at[slot])
            landed(other[k].at[slot], other_l.at[slot])

            @pl.when(t >= 2)
            def _():
                landed(s1[k].at[out], s1_s.at[out])

            def add(rows, cols):
                s1[k][out, 0, rows, cols] = both(k, slot, ox, 0, rows, cols).astype(BF16)
                s1[k][out, 1, rows, cols] = both(k, slot, ox, 1, rows, cols).astype(BF16)
                s1[k][out, 2, rows, cols] = both(k, slot, rx, 1, rows, cols).astype(BF16)
                s1[k][out, 3, rows, cols] = both(k, slot, lx, 0, rows, cols).astype(BF16)

            sweep(k, add)
            remote(s1[k].at[out, 0], hop1[W].at[l, 0, *p], s1_s.at[out], hop1_r.at[t], right).start()
            remote(s1[k].at[out, 1], hop1[W].at[l, 1, *p], s1_s.at[out], hop1_r.at[t], left).start()
            remote(s1[k].at[out, 2], hop2[W].at[l, 0, 1, *p], s1_s.at[out], hop2_r.at[t], right).start()
            remote(s1[k].at[out, 3], hop2[W].at[l, 1, 0, *p], s1_s.at[out], hop2_r.at[t], left).start()

        at(t, go)

    def second(t):
        def go(W, k, l, p):
            slot, out = t % DEPTH, t % 2

            @pl.when(t >= 2)
            def _():
                landed(mb[k].at[out], mv_w.at[out, 0])
                landed(vb[k].at[out], mv_w.at[out, 1])

            local(m[W].at[l, :, *p], mb[k].at[out], mvw_l.at[out, 0]).start()
            local(v[W].at[l, :, *p], vb[k].at[out], mvw_l.at[out, 1]).start()
            local(w[W].at[l, x, c, :, *p], wb[k].at[out], mvw_l.at[out, 2]).start()
            landed(hop1[W].at[l, :, *p], hop1_r.at[t])
            local(hop1[W].at[l, :, *p], r1[k], r1_l).start()

            @pl.when(t >= 2)
            def _():
                landed(s2[k].at[out], s2_s.at[out])

            landed(r1[k], r1_l)

            def add(rows, cols):
                s2[k][out, 0, rows, cols] = (both(k, slot, rx, 0, rows, cols) + r1[k][0, rows, cols].astype(F32)).astype(BF16)
                s2[k][out, 1, rows, cols] = (both(k, slot, lx, 1, rows, cols) + r1[k][1, rows, cols].astype(F32)).astype(BF16)

            sweep(k, add)
            remote(s2[k].at[out, 0], hop2[W].at[l, 0, 0, *p], s2_s.at[out], hop2_r.at[t], right).start()
            remote(s2[k].at[out, 1], hop2[W].at[l, 1, 1, *p], s2_s.at[out], hop2_r.at[t], left).start()

        at(t, go)

    def update(t):
        def go(W, k, l, p):
            slot, out = t % DEPTH, t % 2
            landed(hop2[W].at[l, :, :, *p], hop2_r.at[t])
            local(hop2[W].at[l, :, :, *p], r2[k], r2_l).start()
            landed(mb[k].at[out], mvw_l.at[out, 0])
            landed(vb[k].at[out], mvw_l.at[out, 1])
            landed(wb[k].at[out], mvw_l.at[out, 2])
            landed(r2[k], r2_l)

            def add(rows, cols):
                for h in range(HALVES):
                    place = (out, h, rows, cols)
                    total = both(k, slot, x, h, rows, cols) + r2[k][0, h, rows, cols].astype(F32) + r2[k][1, h, rows, cols].astype(F32)
                    grad = total.astype(BF16).astype(F32)
                    wb[k][place], mb[k][place], vb[k][place] = adamw(wb[k][place].astype(F32), mb[k][place], vb[k][place], grad)

            sweep(k, add)
            mine = w_out[W].at[l, x, c, :, *p]

            local(wb[k].at[out], mine, w_w).start()
            local(mb[k].at[out], m_out[W].at[l, :, *p], mv_w.at[out, 0]).start()
            local(vb[k].at[out], v_out[W].at[l, :, *p], mv_w.at[out, 1]).start()
            landed(wb[k].at[out], w_w)

        at(t, go)

    def spread(t):
        def go(W, l, p, from_left, from_right):
            mine, first, last = w_out[W].at[l, x, c, :, *p], w_out[W].at[l, x, c, 0, *p], w_out[W].at[l, x, c, 1, *p]
            remote(first, from_left, near_s.at[W], near_r.at[t], right).start()
            remote(last, from_right, near_s.at[W], near_r.at[t], left).start()
            remote(last, last, near_s.at[W], near_r.at[t], right).start()
            remote(first, first, near_s.at[W], near_r.at[t], left).start()
            remote(mine, mine, near_s.at[W], core_r.at[W], mate).start()

        near(t, go)

    def relay(t):
        def go(W, l, p, from_left, from_right):
            landed(hop2[W].at[l, :, :, *p], near_r.at[t])
            left0, left1 = w_out[W].at[l, lx, c, 0, *p], w_out[W].at[l, lx, c, 1, *p]
            right0, right1 = w_out[W].at[l, rx, c, 0, *p], w_out[W].at[l, rx, c, 1, *p]
            for src, dst in ((from_left, left0), (left1, left1), (right0, right0), (from_right, right1)):
                remote(src, dst, last_s.at[W], core_r.at[W], mate).start()

        near(t, go)


    load_own(0)
    barrier = pltpu.get_barrier_semaphore()
    for one in (right, left, mate):
        pl.semaphore_signal(barrier, inc=1, device_id=one, device_id_type=MESH)
    pl.semaphore_wait(barrier, 3)

    opening()
    load_other(1)

    def round_(i, _):
        exchange(i + 2)
        load_own(i + 1)
        first(i)
        load_other(i + 1)
        second(i - 1)
        update(i - 2)
        spread(i - 2 - LAG)
        relay(i - 3 - LAG)
        return 0

    lax.fori_loop(1, total + 3 + LAG, round_, 0)

    for t in (total - 2, total - 1):
        landed(s1[1].at[t % 2], s1_s.at[t % 2])
        landed(s2[1].at[t % 2], s2_s.at[t % 2])
        landed(mb[1].at[t % 2], mv_w.at[t % 2, 0])
        landed(vb[1].at[t % 2], mv_w.at[t % 2, 1])
    for W in range(3):
        landed(w_out[W].at[:, pl.ds(0, 3), 0], core_r.at[W])
        landed(pair[W], pair_s.at[W])
        landed(w_out[W].at[:, pl.ds(0, 3), 0], near_s.at[W])
        landed(w_out[W].at[:, pl.ds(0, 2), 0], last_s.at[W])


def moves(sources, results, jobs, given=None):
    count, extra = len(sources), 0 if given is None else 1

    def body(*refs):
        ins, outs = refs[:count], refs[count + extra : count + extra + len(results)]
        bufs, (got, put) = refs[count + extra + len(results) : -2], refs[-2:]
        me = lax.axis_index("dp")
        x, c = me // CORES, me % CORES

        def load(q, i):
            src, _, _, slots, _, _, where = jobs[q]
            return pltpu.make_async_copy(ins[src].at[where(i, x, c)[0]], bufs[q].at[i % slots], got.at[q, i % slots])

        def store(q, i):
            _, dst, _, slots, _, _, where = jobs[q]
            return pltpu.make_async_copy(bufs[q].at[i % slots], outs[dst].at[where(i, x, c)[1]], put.at[q, i % slots])

        for i in range(max(job[4] for job in jobs)):
            for q, job in enumerate(jobs):
                if i < min(job[4], job[2]):
                    load(q, i).start()
        for i in range(max(job[2] for job in jobs)):
            for q, (_, _, steps, slots, ahead, _, _) in enumerate(jobs):
                if i < steps:
                    load(q, i).wait()
                    store(q, i).start()
                    if i + ahead < steps:
                        if i + ahead >= slots:
                            store(q, i + ahead - slots).wait()
                        load(q, i + ahead).start()
        for q, (_, _, steps, slots, _, _, _) in enumerate(jobs):
            for i in range(max(0, steps - slots), steps):
                store(q, i).wait()

    most = max(job[3] for job in jobs)
    hbm = pl.BlockSpec(memory_space=pltpu.HBM)
    nbytes = 2 * sum(job[2] * math.prod(job[5]) * sources[job[0]].dtype.itemsize for job in jobs)
    return pl.pallas_call(
        body,
        in_specs=[hbm] * (count + extra),
        out_specs=[hbm] * len(results),
        out_shape=results,
        scratch_shapes=[pltpu.VMEM((job[3], *job[5]), sources[job[0]].dtype) for job in jobs]
        + [pltpu.SemaphoreType.DMA((len(jobs), most))] * 2,
        input_output_aliases={count: 0} if extra else {},
        compiler_params=pltpu.CompilerParams(vmem_limit_bytes=VMEM),
        cost_estimate=pl.CostEstimate(flops=nbytes * 8, bytes_accessed=nbytes, transcendentals=0),
    )(*sources, *(() if given is None else (given,)))


def solution(mesh):
    n = mesh.shape["dp"]

    def update(*arrays):
        terms, weights, m, v = (arrays[i : i + 3] for i in (0, 3, 6, 9))
        layers = weights[0].shape[0]
        chips = n // CORES
        assert n == CORES * chips and chips == 4
        dims = [(one.shape[1] // HALVES, one.shape[2]) for one in m]

        def whole(one, W):
            return one.reshape(layers, chips, CORES, HALVES, *dims[W])

        def block(one, W):
            return one.reshape(layers, HALVES, *dims[W])

        inputs = (
            [whole(one, W) for W, one in enumerate(terms)]
            + [whole(one, W) for W, one in enumerate(weights)]
            + [block(one, W) for W, one in enumerate(m)]
            + [block(one, W) for W, one in enumerate(v)]
        )

        def outs(*lead, dtype=BF16):
            return [jax.ShapeDtypeStruct((*lead, *dims[W]), dtype) for W in range(3)]

        nears = outs(layers)[:2] + [jax.ShapeDtypeStruct(dims[2], BF16)] * layers
        out_shape = (
            outs(layers, chips, CORES, HALVES)
            + outs(layers, HALVES, dtype=F32)
            + outs(layers, HALVES, dtype=F32)
            + nears * 2
            + outs(layers, chips, HALVES)
            + outs(layers, 2)
            + outs(layers, 2, HALVES)
        )
        tiles = [(dims[0][0], dims[0][1] // SUB), (dims[2][0] // SUB, dims[2][1])]

        def vmem(*lead, dtype=BF16):
            return [pltpu.VMEM((*lead, *tile), dtype) for tile in tiles]

        dma = pltpu.SemaphoreType.DMA
        pieces = 3 * layers * SUB
        scratch = (
            vmem(DEPTH, chips, HALVES)
            + vmem(DEPTH, chips, HALVES)
            + vmem(2)
            + vmem(2, HALVES)
            + vmem(2, 4)
            + vmem(2, 2)
            + vmem(2, HALVES, dtype=F32)
            + vmem(2, HALVES, dtype=F32)
            + vmem(2, HALVES)
            + [dma((pieces,))] * 4
            + [dma((3,)), dma((chips,))]
            + [dma((3,)), dma((2,)), dma((2,)), dma((3,)), dma((3,))]
            + [dma((DEPTH,)), dma((DEPTH,)), dma, dma, dma((2, 3)), dma((2, 2)), dma]
        )
        hbm = pl.BlockSpec(memory_space=pltpu.HBM)
        result = pl.pallas_call(
            functools.partial(kernel, dims, layers, n),
            out_shape=out_shape,
            in_specs=[hbm] * len(inputs),
            out_specs=[hbm] * len(out_shape),
            scratch_shapes=scratch,
            compiler_params=pltpu.CompilerParams(collective_id=0, has_side_effects=True, vmem_limit_bytes=VMEM),
            name="step",
        )(*inputs)
        new_w, new_m, new_v = result[:3], result[3:6], result[6:9]
        of_left, of_right = result[9 : 9 + len(nears)], result[9 + len(nears) : 9 + 2 * len(nears)]

        def moved(one, along, other=False):
            to = [((d // CORES + along) % chips * CORES + (d % CORES + other) % CORES) for d in range(n)]
            return lax.ppermute(one, "dp", list(enumerate(to)))

        def like(one):
            return jax.ShapeDtypeStruct(one.shape, one.dtype)

        every = slice(None)

        def of_blocks(W, src, dst, blocks, half, slots, ahead):
            def where(i, x, c):
                along, other, which = blocks[i // layers]
                place = (i % layers, (x + along) % chips, 1 - c if other else c, which)
                return place, place

            return src, dst, layers * len(blocks), slots, ahead, dims[W] if half else (HALVES, *dims[W]), where

        def of_near(W, src, dst, along, other, half, layer=None, slots=2):
            cuts = 2
            shape = (dims[W][0], dims[W][1] // cuts) if W < 2 else (dims[W][0] // cuts, dims[W][1])

            def where(i, x, c):
                q = i % cuts
                at = (every, pl.ds(q * shape[1], shape[1])) if W < 2 else (pl.ds(q * shape[0], shape[0]), every)
                l = i // cuts if layer is None else layer
                return ((l, *at) if layer is None else at), (l, (x + along) % chips, 1 - c if other else c, half, *at)

            steps = cuts * (layers if layer is None else 1)
            return src, dst, steps, slots, slots // 2, shape, where

        def of_moment(W, src, dst, cuts, slots, ahead):
            shape = (dims[W][0], dims[W][1] // cuts) if W < 2 else (dims[W][0] // cuts, dims[W][1])

            def where(i, x, c):
                q = i % cuts
                at = (every, pl.ds(q * shape[1], shape[1])) if W < 2 else (pl.ds(q * shape[0], shape[0]), every)
                place = (i // (cuts * HALVES), i // cuts % HALVES, *at)
                return place, place

            return src, dst, layers * HALVES * cuts, slots, ahead, shape, where

        def copied(which, new_w, new_m, new_v, of_left, of_right):
            here = [one[W] for one in (new_w, new_m, new_v) for W in which]
            count, jobs, late = len(which), [], []
            for q, W in enumerate(which):
                full = ((0, False, every), (0, True, every), (-1, True, every), (1, True, every))
                jobs.append(of_blocks(W, q, q, full, False, 6, 3))
                jobs.append(of_blocks(W, q, q, ((-1, False, 1), (1, False, 0)), True, 4, 2))
                jobs += [of_moment(W, i, i, 2, 6, 3) for i in (count + q, 2 * count + q)]
                for layer in (None,) if W < 2 else range(layers):
                    at = W + (layer or 0)
                    for one, along, half in ((of_left, -1, 0), (of_right, 1, 1)):
                        jobs.append(of_near(W, len(here) + len(late), q, along, False, half, layer, 4))
                        late.append(one[at])
            return moves((*here, *late), [like(one) for one in here], jobs)

        def placed(W, one, halves):
            jobs = [of_near(W, i, 0, 2, other, half, layer, 4) for i, (_, other, half, layer) in enumerate(halves)]
            return moves([half[0] for half in halves], [like(one)], jobs, one)[0]

        def over(far):
            return [moved(one, 0, True) for one in far]

        def halves(far, mates, layer=None):
            return [(one, other, h, layer) for other, both in ((False, far), (True, mates)) for h, one in enumerate(both)]

        def after(far, which, *others):
            one, others = lax.optimization_barrier((far[which], others))
            return [one if i == which else old for i, old in enumerate(far)], *others

        far = []
        for a, b in zip(of_left, of_right, strict=True):
            far.append((moved(a, 1), moved(b, -1)))
        gate, up, gate_m, up_m, gate_v, up_v = copied((0, 1), new_w, new_m, new_v, of_left, of_right)
        far, _, *rest = after(far, 0, gate_m, new_w, new_m, new_v, of_left, of_right)
        gate_mate = over(far[0])
        down, down_m, down_v = copied((2,), *rest)
        far, gate_mate, _ = after(far, 1, gate_mate, down_m)
        up_mate = over(far[1])
        gate = placed(0, gate, halves(far[0], gate_mate))
        far, up_mate, gate = after(far, 2, up_mate, gate)
        down_mate = over(far[2])
        up = placed(1, up, halves(far[1], up_mate))
        for layer in range(1, layers):
            far, down_mate, up = after(far, 1 + layer, down_mate, up)
            down = placed(2, down, halves(far[1 + layer], down_mate, layer - 1))
            far, down, up = after(far, 2 + layer, down, up)
            down_mate = over(far[2 + layer])
        down = placed(2, down, halves(far[1 + layers], (), layers - 1))
        down = placed(2, down, [(one, True, h, layers - 1) for h, one in enumerate(down_mate)])

        found = (gate, up, down, gate_m, up_m, down_m, gate_v, up_v, down_v)
        return tuple(one.reshape(ref.shape) for one, ref in zip(found, (*weights, *m, *v), strict=True))

    all_of, cut = P(None, None, None), P(None, "dp", None)
    return jax.shard_map(
        update,
        mesh=mesh,
        in_specs=(P(("rep", "dp"), None, None, None),) * 3 + (all_of,) * 3 + (cut,) * 6,
        out_specs=(P("rep", None, None),) * 3 + (P("rep", "dp", None),) * 6,
        check_vma=False,
    )
```

```python
import functools
import math

import jax
import jax.numpy as jnp
from jax import lax
from jax.experimental import pallas as pl
from jax.experimental.pallas import tpu as pltpu
from jax.sharding import PartitionSpec as P


MESH = pl.DeviceIdType.MESH
CORES = 2
HALVES = 2
SUB = 4
DEPTH = 4
LAG = 4
ROWS = 16
VMEM = 67_043_328
BF16, F32 = jnp.bfloat16, jnp.float32


def adamw(w, m, v, g):
    m = 0.9 * m + 0.1 * g
    v = 0.95 * v + 0.05 * g * g
    step = m * lax.rsqrt(v + 1e-8) + 0.1 * w
    return (w - 0.02 * step).astype(jnp.bfloat16), m, v


def kernel(dims, layers, n, groups, *refs):
    kinds = 2
    it = iter(refs)

    def take(count):
        return [next(it) for _ in range(count)]

    g, w, m, v = take(3), take(3), take(3), take(3)
    w_out, m_out, v_out = take(3), take(3), take(3)
    of_left, of_right = take(len(groups)), take(len(groups))
    kept = take(2)
    pair, hop1, hop2 = take(3), take(3), take(3)
    own, other, r1, r2, s1, s2, mb, vb, wb = (take(kinds) for _ in range(9))
    (pair_r, hop1_r, hop2_r, near_r, core_r, open_r) = take(6)
    (pair_s, s1_s, s2_s, near_s, last_s) = take(5)
    (own_l, other_l, r1_l, r2_l, mvw_l, mv_w, w_w) = take(7)

    chips = n // CORES
    me = lax.axis_index("dp")
    x, c = me // CORES, me % CORES
    rx, lx, ox = (x + 1) % chips, (x + chips - 1) % chips, (x + 2) % chips
    right, left, mate = {"dp": rx * CORES + c}, {"dp": lx * CORES + c}, {"dp": x * CORES + 1 - c}

    per = layers * SUB
    total = 3 * per

    def cut(W, j):
        rows, cols = dims[W]
        if W < 2:
            width = cols // SUB
            return slice(None), pl.ds(pl.multiple_of(j * width, 128), width)
        height = rows // SUB
        return pl.ds(pl.multiple_of(j * height, 16), height), slice(None)

    def at(t, f):
        for W in range(3):

            @pl.when((t >= W * per) & (t < (W + 1) * per))
            def _():
                q = t - W * per
                f(W, W // 2, q // SUB, cut(W, q % SUB))

    def near(t, f):
        def go(W, k, l, p):
            if W < 2:
                f(W, l, p, W, (l, *p))
                return
            height = dims[W][0] // SUB
            j = (t - W * per) % SUB
            for number, group in enumerate(groups):
                if group is not None:
                    layer, begin, end = group

                    @pl.when((l == layer) & (j >= begin) & (j < end))
                    def _():
                        f(W, layer, p, number, (pl.ds(pl.multiple_of((j - begin) * height, 16), height), slice(None)))

        at(t, go)

    def remote(src, dst, send, recv, to):
        return pltpu.make_async_remote_copy(src_ref=src, dst_ref=dst, send_sem=send, recv_sem=recv, device_id=to, device_id_type=MESH)

    def local(src, dst, sem):
        return pltpu.make_async_copy(src, dst, sem)

    def landed(ref, sem):
        local(ref, ref, sem).wait()

    def sweep(kind, body):
        height, width = s1[kind].shape[-2:]
        step = width // 3
        across = width // step

        def one(q, _):
            a, b = q // across, q % across
            body(pl.ds(pl.multiple_of(a * ROWS, ROWS), ROWS), pl.ds(pl.multiple_of(b * step, 128), step))
            return 0

        lax.fori_loop(0, (height // ROWS) * across, one, 0)


    def exchange(t):
        def go(W, k, l, p):
            remote(g[W].at[l, :, 1 - c, :, *p], pair[W].at[l, :, :, *p], pair_s.at[W], pair_r.at[t], mate).start()

        at(t, go)

    def load_own(t):
        def go(W, k, l, p):
            local(g[W].at[l, :, c, :, *p], own[k].at[t % DEPTH], own_l.at[t % DEPTH]).start()

        at(t, go)

    def load_other(t):
        def go(W, k, l, p):
            landed(pair[W].at[l, :, :, *p], pair_r.at[t])
            local(pair[W].at[l, :, :, *p], other[k].at[t % DEPTH], other_l.at[t % DEPTH]).start()

        at(t, go)

    def both(k, slot, block, half, rows, cols):
        return own[k][slot, block, half, rows, cols].astype(F32) + other[k][slot, block, half, rows, cols].astype(F32)

    def opening():
        p = cut(0, 0)
        blocks = ((ox, (0, 1)), (rx, (2,)), (lx, (3,)), (x, ()))
        for i, (block, _) in enumerate(blocks):
            remote(g[0].at[0, block, 1 - c, :, *p], other[0].at[0, block], pair_s.at[0], open_r.at[i], mate).start()
        exchange(1)
        exchange(2)
        load_own(1)
        landed(own[0].at[0], own_l.at[0])
        halves = ((ox, 0), (ox, 1), (rx, 1), (lx, 0))
        ends = ((hop1, (0,), hop1_r, right), (hop1, (1,), hop1_r, left), (hop2, (0, 1), hop2_r, right), (hop2, (1, 0), hop2_r, left))
        for i, (block, which) in enumerate(blocks):
            landed(other[0].at[0, block], open_r.at[i])
            if which:

                def add(rows, cols):
                    for q in which:
                        s1[0][0, q, rows, cols] = both(0, 0, *halves[q], rows, cols).astype(BF16)

                sweep(0, add)
            for q in which:
                hop, place, sem, to = ends[q]
                remote(s1[0].at[0, q], hop[0].at[0, *place, *p], s1_s.at[0], sem.at[0], to).start()

    def first(t):
        def go(W, k, l, p):
            slot, out = t % DEPTH, t % 2
            landed(own[k].at[slot], own_l.at[slot])
            landed(other[k].at[slot], other_l.at[slot])

            @pl.when(t >= 2)
            def _():
                landed(s1[k].at[out], s1_s.at[out])

            def add(rows, cols):
                s1[k][out, 0, rows, cols] = both(k, slot, ox, 0, rows, cols).astype(BF16)
                s1[k][out, 1, rows, cols] = both(k, slot, ox, 1, rows, cols).astype(BF16)
                s1[k][out, 2, rows, cols] = both(k, slot, rx, 1, rows, cols).astype(BF16)
                s1[k][out, 3, rows, cols] = both(k, slot, lx, 0, rows, cols).astype(BF16)

            sweep(k, add)
            remote(s1[k].at[out, 0], hop1[W].at[l, 0, *p], s1_s.at[out], hop1_r.at[t], right).start()
            remote(s1[k].at[out, 1], hop1[W].at[l, 1, *p], s1_s.at[out], hop1_r.at[t], left).start()
            remote(s1[k].at[out, 2], hop2[W].at[l, 0, 1, *p], s1_s.at[out], hop2_r.at[t], right).start()
            remote(s1[k].at[out, 3], hop2[W].at[l, 1, 0, *p], s1_s.at[out], hop2_r.at[t], left).start()

        at(t, go)

    def second(t):
        def go(W, k, l, p):
            slot, out = t % DEPTH, t % 2

            @pl.when(t >= 2)
            def _():
                landed(mb[k].at[out], mv_w.at[out, 0])
                landed(vb[k].at[out], mv_w.at[out, 1])

            local(m[W].at[l, :, *p], mb[k].at[out], mvw_l.at[out, 0]).start()
            local(v[W].at[l, :, *p], vb[k].at[out], mvw_l.at[out, 1]).start()
            local(w[W].at[l, x, c, :, *p], wb[k].at[out], mvw_l.at[out, 2]).start()
            landed(hop1[W].at[l, :, *p], hop1_r.at[t])
            local(hop1[W].at[l, :, *p], r1[k], r1_l).start()

            @pl.when(t >= 2)
            def _():
                landed(s2[k].at[out], s2_s.at[out])

            landed(r1[k], r1_l)

            def add(rows, cols):
                s2[k][out, 0, rows, cols] = (both(k, slot, rx, 0, rows, cols) + r1[k][0, rows, cols].astype(F32)).astype(BF16)
                s2[k][out, 1, rows, cols] = (both(k, slot, lx, 1, rows, cols) + r1[k][1, rows, cols].astype(F32)).astype(BF16)

            sweep(k, add)
            remote(s2[k].at[out, 0], hop2[W].at[l, 0, 0, *p], s2_s.at[out], hop2_r.at[t], right).start()
            remote(s2[k].at[out, 1], hop2[W].at[l, 1, 1, *p], s2_s.at[out], hop2_r.at[t], left).start()

        at(t, go)

    def update(t):
        def go(W, k, l, p):
            slot, out = t % DEPTH, t % 2
            landed(hop2[W].at[l, :, :, *p], hop2_r.at[t])
            local(hop2[W].at[l, :, :, *p], r2[k], r2_l).start()
            landed(mb[k].at[out], mvw_l.at[out, 0])
            landed(vb[k].at[out], mvw_l.at[out, 1])
            landed(wb[k].at[out], mvw_l.at[out, 2])
            landed(r2[k], r2_l)

            def add(rows, cols):
                for h in range(HALVES):
                    place = (out, h, rows, cols)
                    total = both(k, slot, x, h, rows, cols) + r2[k][0, h, rows, cols].astype(F32) + r2[k][1, h, rows, cols].astype(F32)
                    grad = total.astype(BF16).astype(F32)
                    wb[k][place], mb[k][place], vb[k][place] = adamw(wb[k][place].astype(F32), mb[k][place], vb[k][place], grad)

            sweep(k, add)
            mine = w_out[W].at[l, x, c, :, *p]

            local(wb[k].at[out], mine, w_w).start()
            local(mb[k].at[out], m_out[W].at[l, :, *p], mv_w.at[out, 0]).start()
            local(vb[k].at[out], v_out[W].at[l, :, *p], mv_w.at[out, 1]).start()
            landed(wb[k].at[out], w_w)

        at(t, go)

    def spread(t):
        def go(W, l, p, number, place):
            mine, first, last = w_out[W].at[l, x, c, :, *p], w_out[W].at[l, x, c, 0, *p], w_out[W].at[l, x, c, 1, *p]
            final = number == len(groups) - 1
            remote(first, of_left[number].at[*place], near_s.at[W], near_r.at[t], right).start()
            remote(last, of_right[number].at[*place], near_s.at[W], near_r.at[t], left).start()
            remote(last, kept[0].at[*place] if final else last, near_s.at[W], near_r.at[t], right).start()
            remote(first, kept[1].at[*place] if final else first, near_s.at[W], near_r.at[t], left).start()
            remote(mine, mine, near_s.at[W], core_r.at[W], mate).start()

        near(t, go)

    def relay(t):
        def go(W, l, p, number, place):
            landed(hop2[W].at[l, :, :, *p], near_r.at[t])
            if number == len(groups) - 1:
                return
            left0, left1 = w_out[W].at[l, lx, c, 0, *p], w_out[W].at[l, lx, c, 1, *p]
            right0, right1 = w_out[W].at[l, rx, c, 0, *p], w_out[W].at[l, rx, c, 1, *p]
            for src, dst in ((of_left[number].at[*place], left0), (left1, left1), (right0, right0), (of_right[number].at[*place], right1)):
                remote(src, dst, last_s.at[W], core_r.at[W], mate).start()

        near(t, go)


    load_own(0)
    barrier = pltpu.get_barrier_semaphore()
    for one in (right, left, mate):
        pl.semaphore_signal(barrier, inc=1, device_id=one, device_id_type=MESH)
    pl.semaphore_wait(barrier, 3)

    opening()
    load_other(1)

    def round_(i, _):
        exchange(i + 2)
        load_own(i + 1)
        first(i)
        load_other(i + 1)
        second(i - 1)
        update(i - 2)
        spread(i - 2 - LAG)
        relay(i - 3 - LAG)
        return 0

    lax.fori_loop(1, total + 3 + LAG, round_, 0)

    for t in (total - 2, total - 1):
        landed(s1[1].at[t % 2], s1_s.at[t % 2])
        landed(s2[1].at[t % 2], s2_s.at[t % 2])
        landed(mb[1].at[t % 2], mv_w.at[t % 2, 0])
        landed(vb[1].at[t % 2], mv_w.at[t % 2, 1])
    for W in range(3):
        final = 0 if W < 2 else groups[-1][2] - groups[-1][1]
        landed(pair[W], pair_s.at[W])
        landed(w_out[W].at[:, pl.ds(0, 3), 0], near_s.at[W])
        if W < 2:
            landed(w_out[W].at[:, pl.ds(0, 3), 0], core_r.at[W])
            landed(w_out[W].at[:, pl.ds(0, 2), 0], last_s.at[W])
        else:
            for sem, count in ((core_r, 3 * per - 2 * final), (last_s, 2 * per - 2 * final)):
                rows = count * (dims[W][0] // SUB) // (layers * chips)
                landed(pair[W].at[:, :, :, pl.ds(0, rows)], sem.at[W])


def moves(sources, results, jobs, given=()):
    count, extra = len(sources), len(given)

    def body(*refs):
        ins, outs = refs[:count], refs[count + extra : count + extra + len(results)]
        bufs, (got, put) = refs[count + extra + len(results) : -2], refs[-2:]
        me = lax.axis_index("dp")
        x, c = me // CORES, me % CORES

        def load(q, i):
            src, _, _, slots, _, _, where = jobs[q]
            return pltpu.make_async_copy(ins[src].at[where(i, x, c)[0]], bufs[q].at[i % slots], got.at[q, i % slots])

        def store(q, i):
            _, dst, _, slots, _, _, where = jobs[q]
            return pltpu.make_async_copy(bufs[q].at[i % slots], outs[dst].at[where(i, x, c)[1]], put.at[q, i % slots])

        for i in range(max(job[4] for job in jobs)):
            for q, job in enumerate(jobs):
                if i < min(job[4], job[2]):
                    load(q, i).start()
        for i in range(max(job[2] for job in jobs)):
            for q, (_, _, steps, slots, ahead, _, _) in enumerate(jobs):
                if i < steps:
                    load(q, i).wait()
                    store(q, i).start()
                    if i + ahead < steps:
                        if i + ahead >= slots:
                            store(q, i + ahead - slots).wait()
                        load(q, i + ahead).start()
        for q, (_, _, steps, slots, _, _, _) in enumerate(jobs):
            for i in range(max(0, steps - slots), steps):
                store(q, i).wait()

    most = max(job[3] for job in jobs)
    hbm = pl.BlockSpec(memory_space=pltpu.HBM)
    nbytes = 2 * sum(job[2] * math.prod(job[5]) * sources[job[0]].dtype.itemsize for job in jobs)
    return pl.pallas_call(
        body,
        in_specs=[hbm] * (count + extra),
        out_specs=[hbm] * len(results),
        out_shape=results,
        scratch_shapes=[pltpu.VMEM((job[3], *job[5]), sources[job[0]].dtype) for job in jobs]
        + [pltpu.SemaphoreType.DMA((len(jobs), most))] * 2,
        input_output_aliases={count + i: i for i in range(extra)},
        compiler_params=pltpu.CompilerParams(vmem_limit_bytes=VMEM),
        cost_estimate=pl.CostEstimate(flops=nbytes * 8, bytes_accessed=nbytes, transcendentals=0),
    )(*sources, *given)


def solution(mesh):
    n = mesh.shape["dp"]

    def update(*arrays):
        terms, weights, m, v = (arrays[i : i + 3] for i in (0, 3, 6, 9))
        layers = weights[0].shape[0]
        chips = n // CORES
        assert n == CORES * chips and chips == 4
        dims = [(one.shape[1] // HALVES, one.shape[2]) for one in m]

        def whole(one, W):
            return one.reshape(layers, chips, CORES, HALVES, *dims[W])

        def block(one, W):
            return one.reshape(layers, HALVES, *dims[W])

        inputs = (
            [whole(one, W) for W, one in enumerate(terms)]
            + [whole(one, W) for W, one in enumerate(weights)]
            + [block(one, W) for W, one in enumerate(m)]
            + [block(one, W) for W, one in enumerate(v)]
        )

        def outs(*lead, dtype=BF16):
            return [jax.ShapeDtypeStruct((*lead, *dims[W]), dtype) for W in range(3)]

        cuts = [(l, 0, SUB) for l in range(layers)]
        groups = [None, None] + cuts
        high = dims[2][0] // SUB
        nears = outs(layers)[:2] + [jax.ShapeDtypeStruct(((end - begin) * high, dims[2][1]), BF16) for _, begin, end in cuts]
        out_shape = (
            outs(layers, chips, CORES, HALVES)
            + outs(layers, HALVES, dtype=F32)
            + outs(layers, HALVES, dtype=F32)
            + nears * 2
            + nears[-1:] * 2
            + outs(layers, chips, HALVES)
            + outs(layers, 2)
            + outs(layers, 2, HALVES)
        )
        tiles = [(dims[0][0], dims[0][1] // SUB), (dims[2][0] // SUB, dims[2][1])]

        def vmem(*lead, dtype=BF16):
            return [pltpu.VMEM((*lead, *tile), dtype) for tile in tiles]

        dma = pltpu.SemaphoreType.DMA
        pieces = 3 * layers * SUB
        scratch = (
            vmem(DEPTH, chips, HALVES)
            + vmem(DEPTH, chips, HALVES)
            + vmem(2)
            + vmem(2, HALVES)
            + vmem(2, 4)
            + vmem(2, 2)
            + vmem(2, HALVES, dtype=F32)
            + vmem(2, HALVES, dtype=F32)
            + vmem(2, HALVES)
            + [dma((pieces,))] * 4
            + [dma((3,)), dma((chips,))]
            + [dma((3,)), dma((2,)), dma((2,)), dma((3,)), dma((3,))]
            + [dma((DEPTH,)), dma((DEPTH,)), dma, dma, dma((2, 3)), dma((2, 2)), dma]
        )
        hbm = pl.BlockSpec(memory_space=pltpu.HBM)
        result = pl.pallas_call(
            functools.partial(kernel, dims, layers, n, groups),
            out_shape=out_shape,
            in_specs=[hbm] * len(inputs),
            out_specs=[hbm] * len(out_shape),
            scratch_shapes=scratch,
            compiler_params=pltpu.CompilerParams(collective_id=0, has_side_effects=True, vmem_limit_bytes=VMEM),
            name="step",
        )(*inputs)
        new_w, new_m, new_v = result[:3], result[3:6], result[6:9]
        of_left, of_right = result[9 : 9 + len(nears)], result[9 + len(nears) : 9 + 2 * len(nears)]
        kept = result[9 + 2 * len(nears) :][:2]

        def moved(one, along, other=False):
            to = [((d // CORES + along) % chips * CORES + (d % CORES + other) % CORES) for d in range(n)]
            return lax.ppermute(one, "dp", list(enumerate(to)))

        def like(one):
            return jax.ShapeDtypeStruct(one.shape, one.dtype)

        every = slice(None)

        def of_blocks(W, src, dst, blocks, half, slots, ahead, spans=None):
            spans = spans or [(l, dims[W][0]) for l in range(layers)]

            def where(i, x, c):
                along, other, which = blocks[i // len(spans)]
                l, rows = spans[i % len(spans)]
                place = (l, (x + along) % chips, 1 - c if other else c, which, slice(0, rows))
                return place, place

            shape = (spans[0][1], dims[W][1])
            return src, dst, len(spans) * len(blocks), slots, ahead, shape if half else (HALVES, *shape), where

        def of_near(number, src, dst, along, other, half, slots=4):
            W, parts = min(number, 2), 2
            l, begin, end = groups[number] or (None, 0, SUB)
            height = (end - begin) * dims[W][0] // SUB
            shape = (height, dims[W][1] // parts) if W < 2 else (height // parts, dims[W][1])

            def where(i, x, c):
                q = i % parts
                to = ((x + along) % chips, 1 - c if other else c, half)
                if W < 2:
                    at = (every, pl.ds(q * shape[1], shape[1]))
                    return (i // parts, *at), (i // parts, *to, *at)
                return (pl.ds(q * shape[0], shape[0]), every), (l, *to, pl.ds(begin * high + q * shape[0], shape[0]), every)

            return src, dst, parts * (layers if W < 2 else 1), slots, slots // 2, shape, where

        def of_moment(W, src, dst, cuts, slots, ahead):
            shape = (dims[W][0], dims[W][1] // cuts) if W < 2 else (dims[W][0] // cuts, dims[W][1])

            def where(i, x, c):
                q = i % cuts
                at = (every, pl.ds(q * shape[1], shape[1])) if W < 2 else (pl.ds(q * shape[0], shape[0]), every)
                place = (i // (cuts * HALVES), i // cuts % HALVES, *at)
                return place, place

            return src, dst, layers * HALVES * cuts, slots, ahead, shape, where

        def copied(which, new_w, new_m, new_v, of_left, of_right, held=()):
            here = [one[W] for one in (new_w, new_m, new_v) for W in which]
            count, jobs, late = len(which), [], []
            for q, W in enumerate(which):
                own, beside = ((0, False, every), (0, True, every)), ((-1, True, every), (1, True, every))
                if W < 2:
                    jobs.append(of_blocks(W, q, q, own + beside, False, 6, 3))
                    jobs.append(of_blocks(W, q, q, ((-1, False, 1), (1, False, 0)), True, 4, 2))
                else:
                    jobs.append(of_blocks(W, q, q, own, False, 4, 2))
                    for span in [(l, dims[W][0]) for l in range(layers - 1)]:
                        jobs.append(of_blocks(W, q, q, beside, False, 2, 2, [span]))
                        jobs.append(of_blocks(W, q, q, ((-1, False, 1), (1, False, 0)), True, 2, 2, [span]))
                jobs += [of_moment(W, i, i, 2, 6, 3) for i in (count + q, 2 * count + q)]
                for number in (W,) if W < 2 else range(2, len(groups)):
                    for one, along, half in ((of_left, -1, 0), (of_right, 1, 1)):
                        jobs.append(of_near(number, len(here) + len(late), q, along, False, half))
                        late.append(one[number])
                for one, place in held:
                    jobs.append(of_near(len(groups) - 1, len(here) + len(late), q, *place))
                    late.append(one)
            return moves((*here, *late), [like(one) for one in here], jobs)

        def placed(given, halves):
            low = min(min(number, 2) for _, number, _, _ in halves)
            jobs = [of_near(number, i, min(number, 2) - low, 2, other, half) for i, (_, number, other, half) in enumerate(halves)]
            return moves([half[0] for half in halves], [like(one) for one in given], jobs, given)

        def over(far):
            return [moved(one, 0, True) for one in far]

        def halves(both, number, other):
            return [(one, number, other, h) for h, one in enumerate(both)]

        def after(far, which, *others):
            one, others = lax.optimization_barrier((far[which], others))
            return [one if i == which else old for i, old in enumerate(far)], *others

        far = []
        for a, b in zip(of_left, of_right, strict=True):
            far.append((moved(a, 1), moved(b, -1)))
        last = len(groups) - 1
        ones = over((of_left[last], kept[0], kept[1], of_right[last]))
        gate, up, gate_m, up_m, gate_v, up_v = copied((0, 1), new_w, new_m, new_v, of_left, of_right)
        far, _, ones, *rest = after(far, 0, gate_m, ones, new_w, new_m, new_v, of_left, of_right)
        gate_mate = over(far[0])
        held = [(one, (along, True, h)) for one, along, h in zip(ones, (-1, -1, 1, 1), (0, 1, 0, 1), strict=True)]
        held += [(kept[0], (-1, False, 1)), (kept[1], (1, False, 0))]
        down, down_m, down_v = copied((2,), *rest, held)
        far, gate_mate, _ = after(far, 1, gate_mate, down_m)
        up_mate = over(far[1])
        far, gate_mate, up_mate = after(far, 2, gate_mate, up_mate)
        mates = over(far[2])
        gate, up = placed((gate, up), halves(far[0], 0, False) + halves(gate_mate, 0, True) + halves(far[1], 1, False) + halves(up_mate, 1, True))
        for number in range(3, len(groups)):
            mates, up = lax.optimization_barrier((mates, up))
            (down,) = placed((down,), halves(far[number - 1], number - 1, False) + halves(mates, number - 1, True))
            far, down, up = after(far, number, down, up)
            mates = over(far[number])
        (down,) = placed((down,), halves(far[last], last, False))
        (down,) = placed((down,), halves(mates, last, True))

        found = (gate, up, down, gate_m, up_m, down_m, gate_v, up_v, down_v)
        return tuple(one.reshape(ref.shape) for one, ref in zip(found, (*weights, *m, *v), strict=True))

    all_of, cut = P(None, None, None), P(None, "dp", None)
    return jax.shard_map(
        update,
        mesh=mesh,
        in_specs=(P(("rep", "dp"), None, None, None),) * 3 + (all_of,) * 3 + (cut,) * 6,
        out_specs=(P("rep", None, None),) * 3 + (P("rep", "dp", None),) * 6,
        check_vma=False,
    )
```

```python
import functools
import math

import jax
import jax.numpy as jnp
from jax import lax
from jax.experimental import pallas as pl
from jax.experimental.pallas import tpu as pltpu
from jax.sharding import PartitionSpec as P


MESH = pl.DeviceIdType.MESH
CORES = 2
HALVES = 2
SUB = 4
DEPTH = 4
LAG = 4
ROWS = 16
VMEM = 67_043_328
BF16, F32 = jnp.bfloat16, jnp.float32


def adamw(w, m, v, g):
    m = 0.9 * m + 0.1 * g
    v = 0.95 * v + 0.05 * g * g
    step = m * lax.rsqrt(v + 1e-8) + 0.1 * w
    return (w - 0.02 * step).astype(jnp.bfloat16), m, v


def kernel(dims, layers, n, groups, *refs):
    kinds = 2
    it = iter(refs)

    def take(count):
        return [next(it) for _ in range(count)]

    g, w, m, v = take(3), take(3), take(3), take(3)
    w_out, m_out, v_out = take(3), take(3), take(3)
    of_left, of_right = take(len(groups)), take(len(groups))
    kept = take(2)
    pair, hop1, hop2 = take(3), take(3), take(3)
    own, other, r1, r2, s1, s2, mb, vb, wb = (take(kinds) for _ in range(9))
    (pair_r, hop1_r, hop2_r, near_r, core_r, open_r) = take(6)
    (pair_s, s1_s, s2_s, near_s, last_s) = take(5)
    (own_l, other_l, r1_l, r2_l, mvw_l, mv_w, w_w) = take(7)

    chips = n // CORES
    me = lax.axis_index("dp")
    x, c = me // CORES, me % CORES
    rx, lx, ox = (x + 1) % chips, (x + chips - 1) % chips, (x + 2) % chips
    right, left, mate = {"dp": rx * CORES + c}, {"dp": lx * CORES + c}, {"dp": x * CORES + 1 - c}

    per = layers * SUB
    total = 3 * per

    def cut(W, j):
        rows, cols = dims[W]
        if W < 2:
            width = cols // SUB
            return slice(None), pl.ds(pl.multiple_of(j * width, 128), width)
        height = rows // SUB
        return pl.ds(pl.multiple_of(j * height, 16), height), slice(None)

    def at(t, f):
        for W in range(3):

            @pl.when((t >= W * per) & (t < (W + 1) * per))
            def _():
                q = t - W * per
                f(W, W // 2, q // SUB, cut(W, q % SUB))

    def near(t, f):
        def go(W, k, l, p):
            if W < 2:
                f(W, l, p, W, (l, *p))
                return
            height = dims[W][0] // SUB
            j = (t - W * per) % SUB
            for number, group in enumerate(groups):
                if group is not None:
                    layer, begin, end = group

                    @pl.when((l == layer) & (j >= begin) & (j < end))
                    def _():
                        f(W, layer, p, number, (pl.ds(pl.multiple_of((j - begin) * height, 16), height), slice(None)))

        at(t, go)

    def remote(src, dst, send, recv, to):
        return pltpu.make_async_remote_copy(src_ref=src, dst_ref=dst, send_sem=send, recv_sem=recv, device_id=to, device_id_type=MESH)

    def local(src, dst, sem):
        return pltpu.make_async_copy(src, dst, sem)

    def landed(ref, sem):
        local(ref, ref, sem).wait()

    def sweep(kind, body):
        height, width = s1[kind].shape[-2:]
        step = width // 3
        across = width // step

        def one(q, _):
            a, b = q // across, q % across
            body(pl.ds(pl.multiple_of(a * ROWS, ROWS), ROWS), pl.ds(pl.multiple_of(b * step, 128), step))
            return 0

        lax.fori_loop(0, (height // ROWS) * across, one, 0)


    def exchange(t):
        def go(W, k, l, p):
            remote(g[W].at[l, :, 1 - c, :, *p], pair[W].at[l, :, :, *p], pair_s.at[W], pair_r.at[t], mate).start()

        at(t, go)

    def load_own(t):
        def go(W, k, l, p):
            local(g[W].at[l, :, c, :, *p], own[k].at[t % DEPTH], own_l.at[t % DEPTH]).start()

        at(t, go)

    def load_other(t):
        def go(W, k, l, p):
            landed(pair[W].at[l, :, :, *p], pair_r.at[t])
            local(pair[W].at[l, :, :, *p], other[k].at[t % DEPTH], other_l.at[t % DEPTH]).start()

        at(t, go)

    def both(k, slot, block, half, rows, cols):
        return own[k][slot, block, half, rows, cols].astype(F32) + other[k][slot, block, half, rows, cols].astype(F32)

    def opening():
        p = cut(0, 0)
        blocks = ((ox, (0, 1)), (rx, (2,)), (lx, (3,)), (x, ()))
        for i, (block, _) in enumerate(blocks):
            remote(g[0].at[0, block, 1 - c, :, *p], other[0].at[0, block], pair_s.at[0], open_r.at[i], mate).start()
        exchange(1)
        exchange(2)
        load_own(1)
        landed(own[0].at[0], own_l.at[0])
        halves = ((ox, 0), (ox, 1), (rx, 1), (lx, 0))
        ends = ((hop1, (0,), hop1_r, right), (hop1, (1,), hop1_r, left), (hop2, (0, 1), hop2_r, right), (hop2, (1, 0), hop2_r, left))
        for i, (block, which) in enumerate(blocks):
            landed(other[0].at[0, block], open_r.at[i])
            if which:

                def add(rows, cols):
                    for q in which:
                        s1[0][0, q, rows, cols] = both(0, 0, *halves[q], rows, cols).astype(BF16)

                sweep(0, add)
            for q in which:
                hop, place, sem, to = ends[q]
                remote(s1[0].at[0, q], hop[0].at[0, *place, *p], s1_s.at[0], sem.at[0], to).start()

    def first(t):
        def go(W, k, l, p):
            slot, out = t % DEPTH, t % 2
            landed(own[k].at[slot], own_l.at[slot])
            landed(other[k].at[slot], other_l.at[slot])

            @pl.when(t >= 2)
            def _():
                landed(s1[k].at[out], s1_s.at[out])

            def add(rows, cols):
                s1[k][out, 0, rows, cols] = both(k, slot, ox, 0, rows, cols).astype(BF16)
                s1[k][out, 1, rows, cols] = both(k, slot, ox, 1, rows, cols).astype(BF16)
                s1[k][out, 2, rows, cols] = both(k, slot, rx, 1, rows, cols).astype(BF16)
                s1[k][out, 3, rows, cols] = both(k, slot, lx, 0, rows, cols).astype(BF16)

            sweep(k, add)
            remote(s1[k].at[out, 0], hop1[W].at[l, 0, *p], s1_s.at[out], hop1_r.at[t], right).start()
            remote(s1[k].at[out, 1], hop1[W].at[l, 1, *p], s1_s.at[out], hop1_r.at[t], left).start()
            remote(s1[k].at[out, 2], hop2[W].at[l, 0, 1, *p], s1_s.at[out], hop2_r.at[t], right).start()
            remote(s1[k].at[out, 3], hop2[W].at[l, 1, 0, *p], s1_s.at[out], hop2_r.at[t], left).start()

        at(t, go)

    def second(t):
        def go(W, k, l, p):
            slot, out = t % DEPTH, t % 2

            @pl.when(t >= 2)
            def _():
                landed(mb[k].at[out], mv_w.at[out, 0])
                landed(vb[k].at[out], mv_w.at[out, 1])

            local(m[W].at[l, :, *p], mb[k].at[out], mvw_l.at[out, 0]).start()
            local(v[W].at[l, :, *p], vb[k].at[out], mvw_l.at[out, 1]).start()
            local(w[W].at[l, x, c, :, *p], wb[k].at[out], mvw_l.at[out, 2]).start()
            landed(hop1[W].at[l, :, *p], hop1_r.at[t])
            local(hop1[W].at[l, :, *p], r1[k], r1_l).start()

            @pl.when(t >= 2)
            def _():
                landed(s2[k].at[out], s2_s.at[out])

            landed(r1[k], r1_l)

            def add(rows, cols):
                s2[k][out, 0, rows, cols] = (both(k, slot, rx, 0, rows, cols) + r1[k][0, rows, cols].astype(F32)).astype(BF16)
                s2[k][out, 1, rows, cols] = (both(k, slot, lx, 1, rows, cols) + r1[k][1, rows, cols].astype(F32)).astype(BF16)

            sweep(k, add)
            remote(s2[k].at[out, 0], hop2[W].at[l, 0, 0, *p], s2_s.at[out], hop2_r.at[t], right).start()
            remote(s2[k].at[out, 1], hop2[W].at[l, 1, 1, *p], s2_s.at[out], hop2_r.at[t], left).start()

        at(t, go)

    def update(t):
        def go(W, k, l, p):
            slot, out = t % DEPTH, t % 2
            landed(hop2[W].at[l, :, :, *p], hop2_r.at[t])
            local(hop2[W].at[l, :, :, *p], r2[k], r2_l).start()
            landed(mb[k].at[out], mvw_l.at[out, 0])
            landed(vb[k].at[out], mvw_l.at[out, 1])
            landed(wb[k].at[out], mvw_l.at[out, 2])
            landed(r2[k], r2_l)

            def add(rows, cols):
                for h in range(HALVES):
                    place = (out, h, rows, cols)
                    total = both(k, slot, x, h, rows, cols) + r2[k][0, h, rows, cols].astype(F32) + r2[k][1, h, rows, cols].astype(F32)
                    grad = total.astype(BF16).astype(F32)
                    wb[k][place], mb[k][place], vb[k][place] = adamw(wb[k][place].astype(F32), mb[k][place], vb[k][place], grad)

            sweep(k, add)
            mine = w_out[W].at[l, x, c, :, *p]

            local(wb[k].at[out], mine, w_w).start()
            local(mb[k].at[out], m_out[W].at[l, :, *p], mv_w.at[out, 0]).start()
            local(vb[k].at[out], v_out[W].at[l, :, *p], mv_w.at[out, 1]).start()
            landed(wb[k].at[out], w_w)

        at(t, go)

    def spread(t):
        def go(W, l, p, number, place):
            mine, first, last = w_out[W].at[l, x, c, :, *p], w_out[W].at[l, x, c, 0, *p], w_out[W].at[l, x, c, 1, *p]
            final = number == len(groups) - 1
            remote(first, of_left[number].at[*place], near_s.at[W], near_r.at[t], right).start()
            remote(last, of_right[number].at[*place], near_s.at[W], near_r.at[t], left).start()
            remote(last, kept[0].at[*place] if final else last, near_s.at[W], near_r.at[t], right).start()
            remote(first, kept[1].at[*place] if final else first, near_s.at[W], near_r.at[t], left).start()
            remote(mine, mine, near_s.at[W], core_r.at[W], mate).start()

        near(t, go)

    def relay(t):
        def go(W, l, p, number, place):
            landed(hop2[W].at[l, :, :, *p], near_r.at[t])
            if number == len(groups) - 1:
                return
            left0, left1 = w_out[W].at[l, lx, c, 0, *p], w_out[W].at[l, lx, c, 1, *p]
            right0, right1 = w_out[W].at[l, rx, c, 0, *p], w_out[W].at[l, rx, c, 1, *p]
            for src, dst in ((of_left[number].at[*place], left0), (left1, left1), (right0, right0), (of_right[number].at[*place], right1)):
                remote(src, dst, last_s.at[W], core_r.at[W], mate).start()

        near(t, go)


    load_own(0)
    barrier = pltpu.get_barrier_semaphore()
    for one in (right, left, mate):
        pl.semaphore_signal(barrier, inc=1, device_id=one, device_id_type=MESH)
    pl.semaphore_wait(barrier, 3)

    opening()
    load_other(1)

    def round_(i, _):
        exchange(i + 2)
        load_own(i + 1)
        first(i)
        load_other(i + 1)
        second(i - 1)
        update(i - 2)
        spread(i - 2 - LAG)
        relay(i - 3 - LAG)
        return 0

    lax.fori_loop(1, total + 3 + LAG, round_, 0)

    for t in (total - 2, total - 1):
        landed(s1[1].at[t % 2], s1_s.at[t % 2])
        landed(s2[1].at[t % 2], s2_s.at[t % 2])
        landed(mb[1].at[t % 2], mv_w.at[t % 2, 0])
        landed(vb[1].at[t % 2], mv_w.at[t % 2, 1])
    for W in range(3):
        final = 0 if W < 2 else groups[-1][2] - groups[-1][1]
        landed(pair[W], pair_s.at[W])
        landed(w_out[W].at[:, pl.ds(0, 3), 0], near_s.at[W])
        if W < 2:
            landed(w_out[W].at[:, pl.ds(0, 3), 0], core_r.at[W])
            landed(w_out[W].at[:, pl.ds(0, 2), 0], last_s.at[W])
        else:
            for sem, count in ((core_r, 3 * per - 2 * final), (last_s, 2 * per - 2 * final)):
                rows = count * (dims[W][0] // SUB) // (layers * chips)
                landed(pair[W].at[:, :, :, pl.ds(0, rows)], sem.at[W])


def moves(sources, results, jobs, given=(), vmem=VMEM):
    count, extra = len(sources), len(given)

    def body(*refs):
        ins, outs = refs[:count], refs[count + extra : count + extra + len(results)]
        bufs, (got, put) = refs[count + extra + len(results) : -2], refs[-2:]
        me = lax.axis_index("dp")
        x, c = me // CORES, me % CORES

        def load(q, i):
            src, _, _, slots, _, _, where = jobs[q]
            return pltpu.make_async_copy(ins[src].at[where(i, x, c)[0]], bufs[q].at[i % slots], got.at[q, i % slots])

        def store(q, i):
            src, dst, _, slots, _, _, where = jobs[q]
            if not slots:
                return pltpu.make_async_copy(ins[src].at[where(i, x, c)[0]], outs[dst].at[where(i, x, c)[1]], put.at[q, i])
            return pltpu.make_async_copy(bufs[q].at[i % slots], outs[dst].at[where(i, x, c)[1]], put.at[q, i % slots])

        for i in range(max(job[2] for job in jobs)):
            for q, job in enumerate(jobs):
                if not job[3] and i < job[2]:
                    store(q, i).start()
                if i < min(job[4], job[2]):
                    load(q, i).start()
        for i in range(max(job[2] for job in jobs)):
            for q, (_, _, steps, slots, ahead, _, _) in enumerate(jobs):
                if slots and i < steps:
                    load(q, i).wait()
                    store(q, i).start()
                    if i + ahead < steps:
                        if i + ahead >= slots:
                            store(q, i + ahead - slots).wait()
                        load(q, i + ahead).start()
        for q, (_, _, steps, slots, _, _, _) in enumerate(jobs):
            for i in range(max(0, steps - slots) if slots else 0, steps):
                store(q, i).wait()

    most = max(job[3] or job[2] for job in jobs)
    inside = {job[0] for job in jobs if not job[3]}
    hbm = pl.BlockSpec(memory_space=pltpu.HBM)
    nbytes = 2 * sum(job[2] * math.prod(job[5]) * sources[job[0]].dtype.itemsize for job in jobs)
    return pl.pallas_call(
        body,
        in_specs=[pl.BlockSpec(memory_space=pltpu.VMEM) if i in inside else hbm for i in range(count)] + [hbm] * extra,
        out_specs=[hbm] * len(results),
        out_shape=results,
        scratch_shapes=[pltpu.VMEM((job[3], *job[5]) if job[3] else (16, 128), sources[job[0]].dtype) for job in jobs]
        + [pltpu.SemaphoreType.DMA((len(jobs), most))] * 2,
        input_output_aliases={count + i: i for i in range(extra)},
        compiler_params=pltpu.CompilerParams(vmem_limit_bytes=vmem),
        cost_estimate=pl.CostEstimate(flops=nbytes * 8, bytes_accessed=nbytes, transcendentals=0),
    )(*sources, *given)


def solution(mesh):
    n = mesh.shape["dp"]

    def update(*arrays):
        terms, weights, m, v = (arrays[i : i + 3] for i in (0, 3, 6, 9))
        layers = weights[0].shape[0]
        chips = n // CORES
        assert n == CORES * chips and chips == 4
        dims = [(one.shape[1] // HALVES, one.shape[2]) for one in m]

        def whole(one, W):
            return one.reshape(layers, chips, CORES, HALVES, *dims[W])

        def block(one, W):
            return one.reshape(layers, HALVES, *dims[W])

        inputs = (
            [whole(one, W) for W, one in enumerate(terms)]
            + [whole(one, W) for W, one in enumerate(weights)]
            + [block(one, W) for W, one in enumerate(m)]
            + [block(one, W) for W, one in enumerate(v)]
        )

        def outs(*lead, dtype=BF16):
            return [jax.ShapeDtypeStruct((*lead, *dims[W]), dtype) for W in range(3)]

        cuts = [(l, 0, SUB) for l in range(layers)]
        groups = [None, None] + cuts
        high = dims[2][0] // SUB
        nears = outs(layers)[:2] + [jax.ShapeDtypeStruct(((end - begin) * high, dims[2][1]), BF16) for _, begin, end in cuts]
        out_shape = (
            outs(layers, chips, CORES, HALVES)
            + outs(layers, HALVES, dtype=F32)
            + outs(layers, HALVES, dtype=F32)
            + nears * 2
            + nears[-1:] * 2
            + outs(layers, chips, HALVES)
            + outs(layers, 2)
            + outs(layers, 2, HALVES)
        )
        tiles = [(dims[0][0], dims[0][1] // SUB), (dims[2][0] // SUB, dims[2][1])]

        def vmem(*lead, dtype=BF16):
            return [pltpu.VMEM((*lead, *tile), dtype) for tile in tiles]

        dma = pltpu.SemaphoreType.DMA
        pieces = 3 * layers * SUB
        scratch = (
            vmem(DEPTH, chips, HALVES)
            + vmem(DEPTH, chips, HALVES)
            + vmem(2)
            + vmem(2, HALVES)
            + vmem(2, 4)
            + vmem(2, 2)
            + vmem(2, HALVES, dtype=F32)
            + vmem(2, HALVES, dtype=F32)
            + vmem(2, HALVES)
            + [dma((pieces,))] * 4
            + [dma((3,)), dma((chips,))]
            + [dma((3,)), dma((2,)), dma((2,)), dma((3,)), dma((3,))]
            + [dma((DEPTH,)), dma((DEPTH,)), dma, dma, dma((2, 3)), dma((2, 2)), dma]
        )
        hbm = pl.BlockSpec(memory_space=pltpu.HBM)
        result = pl.pallas_call(
            functools.partial(kernel, dims, layers, n, groups),
            out_shape=out_shape,
            in_specs=[hbm] * len(inputs),
            out_specs=[hbm] * len(out_shape),
            scratch_shapes=scratch,
            compiler_params=pltpu.CompilerParams(collective_id=0, has_side_effects=True, vmem_limit_bytes=VMEM),
            name="step",
        )(*inputs)
        new_w, new_m, new_v = result[:3], result[3:6], result[6:9]
        of_left, of_right = result[9 : 9 + len(nears)], result[9 + len(nears) : 9 + 2 * len(nears)]
        kept = result[9 + 2 * len(nears) :][:2]

        def moved(one, along, other=False):
            to = [((d // CORES + along) % chips * CORES + (d % CORES + other) % CORES) for d in range(n)]
            return lax.ppermute(one, "dp", list(enumerate(to)))

        def like(one):
            return jax.ShapeDtypeStruct(one.shape, one.dtype)

        every = slice(None)

        def of_blocks(W, src, dst, blocks, half, slots, ahead, spans=None):
            spans = spans or [(l, dims[W][0]) for l in range(layers)]

            def where(i, x, c):
                along, other, which = blocks[i // len(spans)]
                l, rows = spans[i % len(spans)]
                place = (l, (x + along) % chips, 1 - c if other else c, which, slice(0, rows))
                return place, place

            shape = (spans[0][1], dims[W][1])
            return src, dst, len(spans) * len(blocks), slots, ahead, shape if half else (HALVES, *shape), where

        def of_near(number, src, dst, along, other, half, slots=4):
            W, parts = min(number, 2), 2
            l, begin, end = groups[number] or (None, 0, SUB)
            height = (end - begin) * dims[W][0] // SUB
            shape = (height, dims[W][1] // parts) if W < 2 else (height // parts, dims[W][1])

            def where(i, x, c):
                q = i % parts
                to = ((x + along) % chips, 1 - c if other else c, half)
                if W < 2:
                    at = (every, pl.ds(q * shape[1], shape[1]))
                    return (i // parts, *at), (i // parts, *to, *at)
                return (pl.ds(q * shape[0], shape[0]), every), (l, *to, pl.ds(begin * high + q * shape[0], shape[0]), every)

            return src, dst, parts * (layers if W < 2 else 1), slots, slots // 2, shape, where

        def of_moment(W, src, dst, cuts, slots, ahead):
            shape = (dims[W][0], dims[W][1] // cuts) if W < 2 else (dims[W][0] // cuts, dims[W][1])

            def where(i, x, c):
                q = i % cuts
                at = (every, pl.ds(q * shape[1], shape[1])) if W < 2 else (pl.ds(q * shape[0], shape[0]), every)
                place = (i // (cuts * HALVES), i // cuts % HALVES, *at)
                return place, place

            return src, dst, layers * HALVES * cuts, slots, ahead, shape, where

        def copied(which, new_w, new_m, new_v, of_left, of_right, held=()):
            here = [one[W] for one in (new_w, new_m, new_v) for W in which]
            count, jobs, late = len(which), [], []
            for q, W in enumerate(which):
                own, beside = ((0, False, every), (0, True, every)), ((-1, True, every), (1, True, every))
                if W < 2:
                    jobs.append(of_blocks(W, q, q, own + beside, False, 6, 3))
                    jobs.append(of_blocks(W, q, q, ((-1, False, 1), (1, False, 0)), True, 4, 2))
                else:
                    jobs.append(of_blocks(W, q, q, own, False, 4, 2))
                    for span in [(l, dims[W][0]) for l in range(layers - 1)]:
                        jobs.append(of_blocks(W, q, q, beside, False, 2, 2, [span]))
                        jobs.append(of_blocks(W, q, q, ((-1, False, 1), (1, False, 0)), True, 2, 2, [span]))
                jobs += [of_moment(W, i, i, 2, 6, 3) for i in (count + q, 2 * count + q)]
                for number in (W,) if W < 2 else range(2, len(groups)):
                    for one, along, half in ((of_left, -1, 0), (of_right, 1, 1)):
                        jobs.append(of_near(number, len(here) + len(late), q, along, False, half))
                        late.append(one[number])
                for one, place in held:
                    jobs.append(of_near(len(groups) - 1, len(here) + len(late), q, *place))
                    late.append(one)
            return moves((*here, *late), [like(one) for one in here], jobs)

        def placed(given, halves, slots=4, vmem=VMEM):
            low = min(min(number, 2) for _, number, _, _ in halves)
            jobs = [of_near(number, i, min(number, 2) - low, 2, other, half, slots) for i, (_, number, other, half) in enumerate(halves)]
            return moves([half[0] for half in halves], [like(one) for one in given], jobs, given, vmem)

        def over(far):
            return [moved(one, 0, True) for one in far]

        def halves(both, number, other):
            return [(one, number, other, h) for h, one in enumerate(both)]

        def after(far, which, *others):
            one, others = lax.optimization_barrier((far[which], others))
            return [one if i == which else old for i, old in enumerate(far)], *others

        far = []
        for a, b in zip(of_left, of_right, strict=True):
            one = moved(a, 1)
            far.append((one, moved(b, -1)))
        last = len(groups) - 1
        ones = over((of_left[last], kept[0], kept[1], of_right[last]))
        gate, up, gate_m, up_m, gate_v, up_v = copied((0, 1), new_w, new_m, new_v, of_left, of_right)
        far, _, ones, *rest = after(far, 0, gate_m, ones, new_w, new_m, new_v, of_left, of_right)
        gate_mate = over(far[0])
        held = [(one, (along, True, h)) for one, along, h in zip(ones, (-1, -1, 1, 1), (0, 1, 0, 1), strict=True)]
        held += [(kept[0], (-1, False, 1)), (kept[1], (1, False, 0))]
        down, down_m, down_v = copied((2,), *rest, held)
        far, gate_mate, _ = after(far, 1, gate_mate, down_m)
        up_mate = over(far[1])
        (gate,) = placed((gate,), halves(far[0], 0, False) + halves(gate_mate, 0, True))
        far, up_mate, gate = after(far, 2, up_mate, gate)
        mates = over(far[2])
        (up,) = placed((up,), halves(far[1], 1, False) + halves(up_mate, 1, True))
        for number in range(3, len(groups)):
            mates, up = lax.optimization_barrier((mates, up))
            (down,) = placed((down,), halves(far[number - 1], number - 1, False) + halves(mates, number - 1, True))
            far, down, up = after(far, number, down, up)
            mates = over(far[number])
        (down,) = placed((down,), halves(far[last], last, False), vmem=16 * 2**20)
        (down,) = placed((down,), halves(mates, last, True), slots=0, vmem=16 * 2**20)

        found = (gate, up, down, gate_m, up_m, down_m, gate_v, up_v, down_v)
        return tuple(one.reshape(ref.shape) for one, ref in zip(found, (*weights, *m, *v), strict=True))

    all_of, cut = P(None, None, None), P(None, "dp", None)
    return jax.shard_map(
        update,
        mesh=mesh,
        in_specs=(P(("rep", "dp"), None, None, None),) * 3 + (all_of,) * 3 + (cut,) * 6,
        out_specs=(P("rep", None, None),) * 3 + (P("rep", "dp", None),) * 6,
        check_vma=False,
    )
```
